32 devices in a mesh: gx: 16 (over z, y, core), gy: 2 (over x).
Axes of the slice: x: 2, y: 2, z: 4, core: 2. Of those that a mesh axis runs over, the one named last changes fastest.
Arguments:
- populations: float32 [19, 64, 16, 128], P(None, 'gx', 'gy'), may hold values from 0.02 to 0.1
- fluid: int32 [64, 16, 128], P('gx', 'gy'), may hold values 0 or 1
Outputs:
- advanced: float32 [19, 64, 16, 128], P(None, 'gx', 'gy')
The draws below stay inside these ranges and needn't reach their ends.
Inputs may be any that keep to these rules, and one draw needn't show every extreme that they name: 1 marks a fluid cell, 0 a solid one.
All inputs are finite; a program needn't handle non-finite values. No bound on the sum of `fluid` on one device may be relied on, other than what follows from the above.
Results may differ from the reference program's by a relative error of at most 0.0001.
Values sent between devices are 32-bit elements; how exact they have to be, the bound alone decides.
A program may use at most 64 MiB of HBM per device.

```python
import jax
import jax.numpy as jnp
import numpy as np
from jax import lax

NZ = 128
STEPS = 4
NX = 64
NY = 16


def with_ends(values, rng, least, high):
    place = [jax.random.randint(jax.random.fold_in(rng, axis), (), 0, length) for axis, length in enumerate(values.shape)]
    longest = values.shape.index(max(values.shape))
    beside = place[:longest] + [(place[longest] + 1) % values.shape[longest]] + place[longest + 1:]
    return values.at[tuple(place)].set(least).at[tuple(beside)].set(high)


def level_of(own_key, dims, pieces, low, largest):
    loudness = 1.0
    for axis_at, parts in pieces:
        steps = jax.random.uniform(jax.random.fold_in(jax.random.fold_in(own_key, 6), axis_at), (parts,), jnp.float32, low / len(pieces), largest / len(pieces))
        loudness = loudness * jnp.repeat(jnp.exp(steps), dims[axis_at] // parts).reshape((-1,) + (1,) * (len(dims) - 1 - axis_at))
    return loudness


def setup_inputs(seed: int = 0) -> dict:
    keys = jax.random.split(jax.random.key(seed), 3)
    populations = jnp.clip(0.02 + 0.08 * jax.random.uniform(keys[0], (19, NX, NY, NZ), jnp.float32) ** level_of(keys[0], (19, NX, NY, NZ), ((1, 16), (2, 2)), -0.2, 0.2), 0.02, 0.1)
    fluid = with_ends((jax.random.randint(keys[1], (NX, NY, NZ), 0, 8) < 7).astype(jnp.int32), jax.random.fold_in(keys[1], 1), 0, 1)
    return {"populations": populations, "fluid": fluid}


VELOCITIES = np.array([[0, 0, 0], [1, 0, 0], [-1, 0, 0], [0, 1, 0], [0, -1, 0], [0, 0, 1], [0, 0, -1], [1, 1, 0], [-1, -1, 0], [1, -1, 0], [-1, 1, 0], [1, 0, 1], [-1, 0, -1], [1, 0, -1], [-1, 0, 1], [0, 1, 1], [0, -1, -1], [0, 1, -1], [0, -1, 1]])
OPPOSITE = [0, 2, 1, 4, 3, 6, 5, 8, 7, 10, 9, 12, 11, 14, 13, 16, 15, 18, 17]
WEIGHTS = [1.0 / 3.0] + [1.0 / 18.0] * 6 + [1.0 / 36.0] * 12
relax_rate = 1.25


def lattice_step(pops, wet):
    vel = jnp.asarray(VELOCITIES.T.astype(np.float32))
    weights = jnp.asarray(np.array(WEIGHTS, np.float32))
    rho = jnp.sum(pops, axis=0)
    moment = jnp.einsum("dq,qabz->dabz", vel, pops, precision=lax.Precision.HIGHEST)
    speed = moment / rho[None]
    usq = jnp.sum(speed * speed, axis=0)
    proj = jnp.einsum("dq,dabz->qabz", vel, speed, precision=lax.Precision.HIGHEST)
    feq = weights[:, None, None, None] * rho[None] * (1.0 + 3.0 * proj + 4.5 * proj * proj - 1.5 * usq[None])
    post = jnp.where(wet[None], pops + relax_rate * (feq - pops), pops)
    sizea, sizeb = pops.shape[1], pops.shape[2]
    here = wet[1:-1, 1:-1]
    result = []
    for q in range(19):
        cx, cy, cz = int(VELOCITIES[q, 0]), int(VELOCITIES[q, 1]), int(VELOCITIES[q, 2])
        source = jnp.roll(post[q, 1 - cx:sizea - 1 - cx, 1 - cy:sizeb - 1 - cy], cz, axis=-1)
        source_wet = jnp.roll(wet[1 - cx:sizea - 1 - cx, 1 - cy:sizeb - 1 - cy], cz, axis=-1)
        bounced = post[OPPOSITE[q], 1:-1, 1:-1]
        result.append(jnp.where(here, jnp.where(source_wet, source, bounced), post[q, 1:-1, 1:-1]))
    return jnp.stack(result)


def reference(populations, fluid):
    wet = fluid == 1
    current = populations
    for step in range(STEPS):
        padded = jnp.pad(current, ((0, 0), (1, 1), (0, 0), (0, 0)), mode="wrap")
        padded = jnp.pad(padded, ((0, 0), (0, 0), (1, 1), (0, 0)))
        wet_pad = jnp.pad(wet, ((1, 1), (0, 0), (0, 0)), mode="wrap")
        wet_pad = jnp.pad(wet_pad, ((0, 0), (1, 1), (0, 0)))
        current = lattice_step(padded, wet_pad)
    return current
```

```python
import functools

import jax
import jax.numpy as jnp
import numpy as np
from jax import lax
from jax.experimental import pallas as pl
from jax.experimental.pallas import tpu as pltpu
from jax.sharding import PartitionSpec as P

STEPS = 4
DEPTH = 4
PAD = 8
RELAX = 1.25

VEL = [
    (0, 0, 0), (0, 0, 1), (0, 0, -1),
    (0, -1, 0), (0, -1, 1), (0, -1, -1),
    (0, 1, 0), (0, 1, 1), (0, 1, -1),
    (1, 1, 0), (1, 0, 0), (1, 0, 1), (1, 0, -1), (1, -1, 0),
    (-1, -1, 0), (-1, 0, 0), (-1, 0, 1), (-1, 0, -1), (-1, 1, 0),
]
REFERENCE_VEL = [
    (0, 0, 0), (1, 0, 0), (-1, 0, 0), (0, 1, 0), (0, -1, 0), (0, 0, 1), (0, 0, -1),
    (1, 1, 0), (-1, -1, 0), (1, -1, 0), (-1, 1, 0), (1, 0, 1), (-1, 0, -1),
    (1, 0, -1), (-1, 0, 1), (0, 1, 1), (0, -1, -1), (0, 1, -1), (0, -1, 1),
]
TO_REF = [REFERENCE_VEL.index(v) for v in VEL]
OPP = [VEL.index((-x, -y, -z)) for x, y, z in VEL]
WEIGHT = [(1.0 / 3.0, 1.0 / 18.0, 1.0 / 36.0)[abs(x) + abs(y) + abs(z)] for x, y, z in VEL]
DIRECTIONS = [(1, 0), (-1, 0), (0, 1), (0, -1), (1, 1), (1, -1), (-1, 1), (-1, -1)]


def runs(dx, dy):
    picks = [q for q in range(19) if (not dx or VEL[q][0] == dx) and (not dy or VEL[q][1] == dy)]
    result = []
    for q in picks:
        if result and result[-1][1] == q:
            result[-1][1] = q + 1
        else:
            result.append([q, q + 1])
    return result


def spans(d, offset, length, depth):
    if d == 0:
        return [(offset, offset, length, False)]
    inner = depth - 1
    if d > 0:
        full = (offset + length - inner, offset - inner, inner, False)
        edge = (offset + length - depth, offset - depth, 1, True)
    else:
        full = (offset, offset + length, inner, False)
        edge = (offset + inner, offset + length + inner, 1, True)
    return [full, edge] if inner else [edge]


def pieces(dx, dy, sizes, depth):
    lx, ly = sizes
    result = []
    for xs, xt, xn, xedge in spans(dx, depth, lx, depth):
        for ys, yt, yn, yedge in spans(dy, PAD, ly, depth):
            for lo, hi in runs(dx if xedge else 0, dy if yedge else 0):
                result.append((lo, hi - lo, xs, xt, xn, ys, yt, yn))
    return result


def mark_piece(dx, dy, sizes, depth):
    def along(d, offset, length):
        if d == 0:
            return offset, offset, length
        if d > 0:
            return offset + length - depth, offset - depth, depth
        return offset, offset + length, depth

    return along(dx, depth, sizes[0]) + along(dy, PAD, sizes[1])


def collide(f):
    pairs = [(q, OPP[q]) for q in range(1, 19) if q < OPP[q]]
    rho = f[0]
    moment = [None, None, None]
    for i, j in pairs:
        rho = rho + (f[i] + f[j])
        diff = f[i] - f[j]
        for axis in range(3):
            c = VEL[i][axis]
            if c:
                term = moment[axis]
                if term is None:
                    moment[axis] = diff if c > 0 else -diff
                else:
                    moment[axis] = term + diff if c > 0 else term - diff
    inverse = 1.0 / rho
    u = [m * inverse for m in moment]
    base = 1.0 - 1.5 * (u[0] * u[0] + u[1] * u[1] + u[2] * u[2])
    scaled = {w: (RELAX * w) * rho for w in set(WEIGHT)}
    keep = 1.0 - RELAX
    post = [None] * 19
    post[0] = keep * f[0] + scaled[WEIGHT[0]] * base
    for i, j in pairs:
        proj = None
        for axis in range(3):
            c = VEL[i][axis]
            if c:
                if proj is None:
                    proj = u[axis] if c > 0 else -u[axis]
                else:
                    proj = proj + u[axis] if c > 0 else proj - u[axis]
        even = scaled[WEIGHT[i]] * (base + 4.5 * (proj * proj))
        odd = scaled[WEIGHT[i]] * (3.0 * proj)
        post[i] = keep * f[i] + (even + odd)
        post[j] = keep * f[j] + (even - odd)
    return post


def row_starts(ring, ly):
    first, last = PAD - ring, PAD + ly + ring
    starts = list(range(first, last - 7, 8))
    if starts[-1] + 8 < last:
        starts.append(last - 8)
    return starts


def stream(buf, marks, layer, row):
    result = []
    for q, (cx, cy, cz) in enumerate(VEL):
        if q == 0:
            result.append(buf[0, layer, pl.ds(row, 8), :])
            continue
        source = buf[q, layer - cx, pl.ds(row - cy, 8), :]
        if cz:
            source = pltpu.roll(source, cz % source.shape[-1], 1)
        open_ = marks[cz % 3, layer - cx, pl.ds(row - cy, 8), :] != 0
        result.append(jnp.where(open_, source, buf[OPP[q], layer, pl.ds(row, 8), :]))
    return result


def kernel(axes, sizes, depth, pops_hbm, fluid_hbm, out_hbm, first, last_f, marks, *rest):
    rounds = STEPS // depth
    bufs, rest = rest[:rounds], rest[rounds:]
    inner, rest = rest[: depth - 1], rest[depth - 1 :]
    in_sem, out_sem, mark_send, mark_recv, send_sem, recv_sem = rest
    lx, ly = sizes
    nx, ny = axes
    ix, iy = lax.axis_index("gx"), lax.axis_index("gy")
    has = {0: None, 1: iy < ny - 1, -1: iy > 0}

    def when(condition, action):
        if condition is None:
            action()
        else:
            pl.when(condition)(action)

    def target(dx, dy):
        return {"gx": lax.rem(ix + nx + dx, nx), "gy": iy + dy}

    fluid_in = pltpu.make_async_copy(
        fluid_hbm, marks.at[0, pl.ds(depth, lx), pl.ds(PAD, ly)], in_sem.at[lx]
    )
    loads = [
        pltpu.make_async_copy(pops_hbm.at[:, a], first.at[:, a], in_sem.at[a]) for a in range(lx)
    ]

    barrier = pltpu.get_barrier_semaphore()
    for dx, dy in DIRECTIONS:
        when(
            has[dy],
            lambda dx=dx, dy=dy: pl.semaphore_signal(
                barrier, inc=1, device_id=target(dx, dy), device_id_type=pl.DeviceIdType.MESH
            ),
        )

    fluid_in.start()
    for load in loads:
        load.start()

    for edge, rows in ((iy == 0, PAD - depth), (iy == ny - 1, PAD + ly)):

        @pl.when(edge)
        def _():
            for a in range(lx + 2 * depth):
                marks[0, a, rows : rows + depth, :] = jnp.zeros((depth, marks.shape[-1]), jnp.int32)

    def post_layer(a):
        f = [first[TO_REF[q], a] for q in range(19)]
        for q, value in enumerate(collide(f)):
            bufs[0][q, depth + a, PAD : PAD + ly, :] = value

    order = sorted(range(lx), key=lambda a: min(a, lx - 1 - a))
    for a in order:
        loads[a].wait()
        post_layer(a)
    fluid_in.wait()

    peers = 2 + 3 * (iy > 0).astype(jnp.int32) + 3 * (iy < ny - 1).astype(jnp.int32)
    pl.semaphore_wait(barrier, peers)

    def exchange(copies):
        for (dx, dy), group in copies:
            when(has[dy], lambda group=group: [c.start() for c in group] and None)

    def arrive(copies):
        for (dx, dy), group in copies:
            when(has[-dy], lambda group=group: [c.wait_recv() for c in group] and None)

    def drain(copies):
        for (dx, dy), group in copies:
            when(has[dy], lambda group=group: [c.wait_send() for c in group] and None)

    def mark_copies():
        result = []
        for i, (dx, dy) in enumerate(DIRECTIONS):
            xs, xt, xn, ys, yt, yn = mark_piece(dx, dy, sizes, depth)
            result.append(
                (
                    (dx, dy),
                    [
                        pltpu.make_async_remote_copy(
                            src_ref=marks.at[0, pl.ds(xs, xn), pl.ds(ys, yn)],
                            dst_ref=marks.at[0, pl.ds(xt, xn), pl.ds(yt, yn)],
                            send_sem=mark_send.at[i],
                            recv_sem=mark_recv.at[i],
                            device_id=target(dx, dy),
                            device_id_type=pl.DeviceIdType.MESH,
                        )
                    ],
                )
            )
        return result

    def halo_copies(turn):
        buf = bufs[turn]
        result, count = [], 0
        for dx, dy in DIRECTIONS:
            group = []
            for lo, n, xs, xt, xn, ys, yt, yn in pieces(dx, dy, sizes, depth):
                group.append(
                    pltpu.make_async_remote_copy(
                        src_ref=buf.at[pl.ds(lo, n), pl.ds(xs, xn), pl.ds(ys, yn)],
                        dst_ref=buf.at[pl.ds(lo, n), pl.ds(xt, xn), pl.ds(yt, yn)],
                        send_sem=send_sem.at[turn, count],
                        recv_sem=recv_sem.at[turn, count],
                        device_id=target(dx, dy),
                        device_id_type=pl.DeviceIdType.MESH,
                    )
                )
                count += 1
            result.append(((dx, dy), group))
        return result

    mark_list = mark_copies()
    exchange(mark_list)
    halos = [halo_copies(turn) for turn in range(rounds)]
    exchange(halos[0])

    arrive(mark_list)
    for a in range(lx + 2 * depth):
        for row in row_starts(depth, ly):
            here = marks[0, a, row : row + 8, :]
            lanes = here.shape[-1]
            marks[1, a, row : row + 8, :] = pltpu.roll(here, 1, 1)
            marks[2, a, row : row + 8, :] = pltpu.roll(here, lanes - 1, 1)

    stores = []
    for turn in range(rounds):
        arrive(halos[turn])
        source = bufs[turn]
        for ring in range(depth - 1, -1, -1):
            final = turn == rounds - 1 and ring == 0
            for a in range(-ring, lx + ring):
                for row in row_starts(ring, ly):
                    f = stream(source, marks, depth + a, row)
                    if final:
                        wet = marks[0, depth + a, row : row + 8, :] != 0
                        for q in range(19):
                            old = first[TO_REF[q], a, row - PAD : row - PAD + 8, :]
                            out_hbm[TO_REF[q], a, row - PAD : row - PAD + 8, :] = jnp.where(
                                wet, f[q], old
                            )
                    else:
                        into = inner[ring - 1] if ring else bufs[turn + 1]
                        for q, value in enumerate(collide(f)):
                            into[q, depth + a, row : row + 8, :] = value
                if final:
                    store = None
            if ring:
                source = inner[ring - 1]
        if turn + 1 < rounds:
            exchange(halos[turn + 1])
    drain(mark_list)
    for turn in range(rounds):
        drain(halos[turn])
    for store in stores:
        store.wait()


def per_device(axes, depth, populations, fluid):
    sizes = fluid.shape[:2]
    lx, ly = sizes
    nz = fluid.shape[2]
    rounds = STEPS // depth
    wide = (lx + 2 * depth, ly + 2 * PAD, nz)
    count = sum(len(pieces(dx, dy, sizes, depth)) for dx, dy in DIRECTIONS)
    dma = pltpu.SemaphoreType.DMA
    mid = pl.pallas_call(
        functools.partial(kernel, axes, sizes, depth),
        out_shape=pltpu.VMEM(populations.shape, populations.dtype),
        in_specs=[pl.BlockSpec(memory_space=pl.ANY)] * 2,
        out_specs=pl.BlockSpec(memory_space=pltpu.VMEM),
        scratch_shapes=[
            pltpu.VMEM(populations.shape, jnp.float32),
            pltpu.VMEM(populations.shape, jnp.float32),
            pltpu.VMEM((3,) + wide, jnp.int32),
        ]
        + [pltpu.VMEM((19,) + wide, jnp.float32)] * (rounds + depth - 1)
        + [
            dma((lx + 1,)),
            dma((lx,)),
            dma((len(DIRECTIONS),)),
            dma((len(DIRECTIONS),)),
            dma((rounds, count)),
            dma((rounds, count)),
        ],
        compiler_params=pltpu.CompilerParams(collective_id=0, has_side_effects=True, vmem_limit_bytes=60 * 1024 * 1024),
    )(populations, fluid)
    def k2(x, o, sem):
        cs=[pltpu.make_async_copy(x.at[:, a], o.at[:, a], sem.at[a]) for a in range(lx)]
        for c in cs: c.start()
        for c in cs: c.wait()
    return pl.pallas_call(k2, out_shape=jax.ShapeDtypeStruct(populations.shape, populations.dtype),
        in_specs=[pl.BlockSpec(memory_space=pltpu.VMEM)], out_specs=pl.BlockSpec(memory_space=pl.ANY),
        scratch_shapes=[dma((lx,))], compiler_params=pltpu.CompilerParams(vmem_limit_bytes=16*2**20))(mid)


def solution(mesh):
    axes = (mesh.shape["gx"], mesh.shape["gy"])
    return jax.shard_map(
        functools.partial(per_device, axes, DEPTH),
        mesh=mesh,
        in_specs=(P(None, "gx", "gy", None), P("gx", "gy", None)),
        out_specs=P(None, "gx", "gy", None),
        check_vma=False,
    )
```

```python
import functools

import jax
import jax.numpy as jnp
import numpy as np
from jax import lax
from jax.experimental import pallas as pl
from jax.experimental.pallas import tpu as pltpu
from jax.sharding import PartitionSpec as P

STEPS = 4
HALO = 4
PAD = 8
RELAX = 1.25

VEL = [
    (0, 0, 0), (0, 0, 1), (0, 0, -1),
    (0, -1, 0), (0, -1, 1), (0, -1, -1),
    (0, 1, 0), (0, 1, 1), (0, 1, -1),
    (1, 1, 0), (1, 0, 0), (1, 0, 1), (1, 0, -1), (1, -1, 0),
    (-1, -1, 0), (-1, 0, 0), (-1, 0, 1), (-1, 0, -1), (-1, 1, 0),
]
REFERENCE_VEL = [
    (0, 0, 0), (1, 0, 0), (-1, 0, 0), (0, 1, 0), (0, -1, 0), (0, 0, 1), (0, 0, -1),
    (1, 1, 0), (-1, -1, 0), (1, -1, 0), (-1, 1, 0), (1, 0, 1), (-1, 0, -1),
    (1, 0, -1), (-1, 0, 1), (0, 1, 1), (0, -1, -1), (0, 1, -1), (0, -1, 1),
]
TO_REF = [REFERENCE_VEL.index(v) for v in VEL]
OPP = [VEL.index((-x, -y, -z)) for x, y, z in VEL]
WEIGHT = [(1.0 / 3.0, 1.0 / 18.0, 1.0 / 36.0)[abs(x) + abs(y) + abs(z)] for x, y, z in VEL]
DIRECTIONS = [(1, 0), (-1, 0), (0, 1), (0, -1), (1, 1), (1, -1), (-1, 1), (-1, -1)]


def pieces(dx, dy, sizes):
    lx, ly = sizes

    def beyond(d, length, near, far):
        return (-far if d > 0 else length - 1 + near, far - near + 1)

    def x(near, far=None):
        return beyond(dx, lx, near, far or near)

    def y(near, far=None):
        return beyond(dy, ly, near, far or near)

    def one(cx, cy):
        return VEL.index((cx, cy, 0)), 1

    every = (0, 19)
    if dy == 0:
        cells = [
            (1, every, x(1), (0, ly)),
            (1, every, x(2, 3), (0, 1)),
            (1, every, x(2, 3), (ly - 1, 1)),
            (1, one(dx, -1), x(4), (0, 1)),
            (1, one(dx, 1), x(4), (ly - 1, 1)),
            (2, every, x(2), (1, ly - 2)),
            (2, one(dx, -1), x(3), (1, 1)),
            (2, one(dx, 1), x(3), (ly - 2, 1)),
        ]
    elif dx == 0:
        cells = [
            (1, every, (0, lx), y(1)),
            (1, every, (0, 1), y(2, 3)),
            (1, every, (lx - 1, 1), y(2, 3)),
            (1, one(-1, dy), (0, 1), y(4)),
            (1, one(1, dy), (lx - 1, 1), y(4)),
            (2, every, (1, lx - 2), y(2)),
            (2, one(-1, dy), (1, 1), y(3)),
            (2, one(1, dy), (lx - 2, 1), y(3)),
        ]
    else:
        cells = [
            (1, every, x(1), y(1, 3)),
            (1, every, x(2, 3), y(1)),
            (1, one(dx, dy), x(4), y(1)),
            (1, one(dx, dy), x(1), y(4)),
            (2, every, x(2), y(2)),
            (2, one(dx, dy), x(3), y(2)),
            (2, one(dx, dy), x(2), y(3)),
        ]
    return [(level, lo, n, layers, rows) for level, (lo, n), layers, rows in cells]


def place(a, b, sizes):
    lx, ly = sizes
    bx = (a >= lx) - (a < 0)
    by = (b >= ly) - (b < 0)
    a, b = a - bx * lx, b - by * ly
    return (bx, by), min(a + 1, lx - a, b + 1, ly - b, 2)


def linked(time, sizes):
    def rule(x, y):
        if time > 2:
            return True
        block, level = place(*x, sizes)
        other, beneath = place(*y, sizes)
        return block != other or block == (0, 0) or level < time or beneath < time

    return rule


def linked_inside(time, sizes):
    def rule(x, y):
        block, level = place(*y, sizes)
        return block == (0, 0) and level >= time

    return rule


def collide(f):
    pairs = [(q, OPP[q]) for q in range(1, 19) if q < OPP[q]]
    rho = f[0]
    moment = [None, None, None]
    for i, j in pairs:
        rho = rho + (f[i] + f[j])
        diff = f[i] - f[j]
        for axis in range(3):
            c = VEL[i][axis]
            if c:
                term = moment[axis]
                if term is None:
                    moment[axis] = diff if c > 0 else -diff
                else:
                    moment[axis] = term + diff if c > 0 else term - diff
    inverse = 1.0 / rho
    u = [m * inverse for m in moment]
    base = 1.0 - 1.5 * (u[0] * u[0] + u[1] * u[1] + u[2] * u[2])
    scaled = {w: (RELAX * w) * rho for w in set(WEIGHT)}
    keep = 1.0 - RELAX
    post = [None] * 19
    post[0] = keep * f[0] + scaled[WEIGHT[0]] * base
    for i, j in pairs:
        proj = None
        for axis in range(3):
            c = VEL[i][axis]
            if c:
                if proj is None:
                    proj = u[axis] if c > 0 else -u[axis]
                else:
                    proj = proj + u[axis] if c > 0 else proj - u[axis]
        even = scaled[WEIGHT[i]] * (base + 4.5 * (proj * proj))
        odd = scaled[WEIGHT[i]] * (3.0 * proj)
        post[i] = keep * f[i] + (even + odd)
        post[j] = keep * f[j] + (even - odd)
    return post


def stream(buf, corner, a, row, rule):
    layer, base = corner[0] + a, corner[1] + row
    shape = (8, buf.shape[-1])
    rows = lax.broadcasted_iota(jnp.int32, shape, 0)
    masks = {}

    def open_rows(pattern):
        if pattern not in masks:
            mask = None
            start = 0
            while start < 8:
                if pattern[start]:
                    end = start
                    while end < 8 and pattern[end]:
                        end += 1
                    part = None
                    if start > 0:
                        part = rows >= start
                    if end < 8:
                        part = rows < end if part is None else part & (rows < end)
                    mask = part if mask is None else mask | part
                    start = end
                else:
                    start += 1
            masks[pattern] = mask
        return masks[pattern]

    result = []
    for q, (cx, cy, cz) in enumerate(VEL):
        kept = buf[OPP[q], layer, base : base + 8, :]
        pattern = tuple(rule((a, row + r), (a - cx, row + r - cy)) for r in range(8))
        if q == 0 or not any(pattern):
            result.append(kept)
            continue
        source = buf[q, layer - cx, base - cy : base - cy + 8, :]
        if cz:
            source = pltpu.roll(source, cz % source.shape[-1], 1)
        carry = source == source
        if not all(pattern):
            carry = carry & open_rows(pattern)
        result.append(jnp.where(carry, source, kept))
    return result


def kernel(axes, sizes, pops_hbm, fluid_hbm, out, first, wet, own1, own2, s1, s2, p1, p2, p3, p4, *sems):
    in_sem, send_sem, recv_sem = sems
    lx, ly = sizes
    nx, ny = axes
    ix, iy = lax.axis_index("gx"), lax.axis_index("gy")
    has = {0: None, 1: iy < ny - 1, -1: iy > 0}
    lanes = first.shape[-1]
    solid = jnp.full((ly, lanes), jnp.nan, jnp.float32)

    def when(condition, action):
        if condition is None:
            action()
        else:
            pl.when(condition)(action)

    def target(dx, dy):
        return {"gx": lax.rem(ix + nx + dx, nx), "gy": iy + dy}

    fluid_in = pltpu.make_async_copy(fluid_hbm, wet, in_sem.at[lx])
    loads = [
        pltpu.make_async_copy(pops_hbm.at[:, a], first.at[:, a], in_sem.at[a]) for a in range(lx)
    ]

    barrier = pltpu.get_barrier_semaphore()
    for dx, dy in DIRECTIONS:
        when(
            has[dy],
            lambda dx=dx, dy=dy: pl.semaphore_signal(
                barrier, inc=1, device_id=target(dx, dy), device_id_type=pl.DeviceIdType.MESH
            ),
        )

    fluid_in.start()
    for load in loads:
        load.start()

    for edge, row in ((iy == 0, PAD - 8), (iy == ny - 1, PAD + ly)):

        @pl.when(edge)
        def _():
            for q in range(19):
                for a in range(lx + 2 * HALO):
                    p1[q, a, row : row + 8, :] = jnp.full((8, lanes), jnp.nan, jnp.float32)

    def message(level, dx, dy):
        source, into = ((s1, p1), (s2, p2))[level - 1]
        base = sum(len(pieces(*d, sizes)) for d in DIRECTIONS[: DIRECTIONS.index((dx, dy))])
        copies = []
        for i, (at, lo, n, (a, an), (b, bn)) in enumerate(pieces(dx, dy, sizes)):
            if at == level:
                copies.append(
                    pltpu.make_async_remote_copy(
                        src_ref=source.at[pl.ds(lo, n), pl.ds(a + dx * lx, an), pl.ds(b + dy * ly, bn)],
                        dst_ref=into.at[pl.ds(lo, n), pl.ds(HALO + a, an), pl.ds(PAD + b, bn)],
                        send_sem=send_sem.at[base + i],
                        recv_sem=recv_sem.at[base + i],
                        device_id=target(dx, dy),
                        device_id_type=pl.DeviceIdType.MESH,
                    )
                )
        return copies

    def each(condition, copies, action):
        when(condition, lambda: [getattr(c, action)() for c in copies] and None)

    fluid_in.wait()
    for a in sorted(range(lx), key=lambda a: min(a, lx - 1 - a)):
        loads[a].wait()
        f = [first[TO_REF[q], a] for q in range(19)]
        f[0] = jnp.where(wet[a] != 0, f[0], solid)
        for q, value in enumerate(collide(f)):
            own1[q, a, PAD : PAD + ly, :] = value
            p1[q, HALO + a, PAD : PAD + ly, :] = value

    def part(source, into, a, time):
        f = stream(source, (0, PAD), a, 0, linked_inside(time, sizes))
        for q, value in enumerate(f):
            into[OPP[q], a] = jnp.where(wet[a] != 0, value, solid)
        return f

    for a in range(lx):
        f = part(own1, s1, a, 1)
        if 0 < a < lx - 1:
            for q, value in enumerate(collide(f)):
                own2[q, a, PAD : PAD + ly, :] = value

    peers = 2 + 3 * (iy > 0).astype(jnp.int32) + 3 * (iy < ny - 1).astype(jnp.int32)
    pl.semaphore_wait(barrier, peers)
    for d in DIRECTIONS:
        each(has[d[1]], message(1, *d), "start")
    for a in range(1, lx - 1):
        part(own2, s2, a, 2)
    for d in DIRECTIONS:
        each(has[d[1]], message(2, *d), "start")

    def advance(source, into, time, a, row, lo=0, hi=8):
        f = stream(source, (HALO, PAD), a, row, linked(time, sizes))
        for q, value in enumerate(collide(f)):
            into[q, HALO + a, PAD + row + lo : PAD + row + hi, :] = value[lo:hi]

    def rows(ring):
        return sorted({-ring, ly + ring - 8})

    for d in DIRECTIONS:
        each(has[-d[1]], message(1, *d), "wait_recv")
    for a in range(lx):
        for row in rows(3 if a in (0, lx - 1) else 1):
            advance(p1, p2, 1, a, row)
    for a in (-1, lx):
        for row in rows(3):
            advance(p1, p2, 1, a, row)
    for a in (-3, -2, lx + 1, lx + 2):
        advance(p1, p2, 1, a, -1, 0, 2)
        advance(p1, p2, 1, a, ly - 7, 6, 8)
    for d in DIRECTIONS:
        each(has[-d[1]], message(2, *d), "wait_recv")
    for a in range(-2, lx + 2):
        for row in rows(2):
            advance(p2, p3, 2, a, row)
    for a in range(-1, lx + 1):
        for row in rows(1):
            advance(p3, p4, 3, a, row)
    for a in range(lx):
        f = stream(p4, (HALO, PAD), a, 0, linked(4, sizes))
        for q in range(19):
            out[TO_REF[q], a] = jnp.where(wet[a] != 0, f[q], first[TO_REF[q], a])
    for level in (1, 2):
        for d in DIRECTIONS:
            each(has[d[1]], message(level, *d), "wait_send")


def write_out(source, target, sem):
    copies = [
        pltpu.make_async_copy(source.at[:, a], target.at[:, a], sem.at[a])
        for a in range(source.shape[1])
    ]
    for copy in copies:
        copy.start()
    for copy in copies:
        copy.wait()


def per_device(axes, populations, fluid):
    sizes = fluid.shape[:2]
    lx, ly = sizes
    nz = fluid.shape[2]
    count = sum(len(pieces(dx, dy, sizes)) for dx, dy in DIRECTIONS)
    dma = pltpu.SemaphoreType.DMA
    block = pltpu.VMEM(populations.shape, jnp.float32)
    tall = pltpu.VMEM((19, lx, ly + 2 * PAD, nz), jnp.float32)
    wide = pltpu.VMEM((19, lx + 2 * HALO, ly + 2 * PAD, nz), jnp.float32)
    result = pl.pallas_call(
        functools.partial(kernel, axes, sizes),
        out_shape=pltpu.VMEM(populations.shape, populations.dtype),
        in_specs=[pl.BlockSpec(memory_space=pl.ANY)] * 2,
        out_specs=pl.BlockSpec(memory_space=pltpu.VMEM),
        scratch_shapes=[block, pltpu.VMEM(fluid.shape, jnp.int32), tall, tall, block, block]
        + [wide] * STEPS
        + [dma((lx + 1,)), dma((count,)), dma((count,))],
        compiler_params=pltpu.CompilerParams(
            collective_id=0, has_side_effects=True, vmem_limit_bytes=60 * 1024 * 1024
        ),
    )(populations, fluid)
    return pl.pallas_call(
        write_out,
        out_shape=jax.ShapeDtypeStruct(populations.shape, populations.dtype),
        in_specs=[pl.BlockSpec(memory_space=pltpu.VMEM)],
        out_specs=pl.BlockSpec(memory_space=pl.ANY),
        scratch_shapes=[dma((lx,))],
        compiler_params=pltpu.CompilerParams(vmem_limit_bytes=16 * 2**20),
    )(result)


def solution(mesh):
    axes = (mesh.shape["gx"], mesh.shape["gy"])
    return jax.shard_map(
        functools.partial(per_device, axes),
        mesh=mesh,
        in_specs=(P(None, "gx", "gy", None), P("gx", "gy", None)),
        out_specs=P(None, "gx", "gy", None),
        check_vma=False,
    )
```

```python
import functools

import jax
import jax.numpy as jnp
import numpy as np
from jax import lax
from jax.experimental import pallas as pl
from jax.experimental.pallas import tpu as pltpu
from jax.sharding import PartitionSpec as P

STEPS = 4
HALO = 4
PAD = 8
RELAX = 1.25

VEL = [
    (0, 0, 0), (0, 0, 1), (0, 0, -1),
    (0, -1, 0), (0, -1, 1), (0, -1, -1),
    (0, 1, 0), (0, 1, 1), (0, 1, -1),
    (1, 1, 0), (1, 0, 0), (1, 0, 1), (1, 0, -1), (1, -1, 0),
    (-1, -1, 0), (-1, 0, 0), (-1, 0, 1), (-1, 0, -1), (-1, 1, 0),
]
REFERENCE_VEL = [
    (0, 0, 0), (1, 0, 0), (-1, 0, 0), (0, 1, 0), (0, -1, 0), (0, 0, 1), (0, 0, -1),
    (1, 1, 0), (-1, -1, 0), (1, -1, 0), (-1, 1, 0), (1, 0, 1), (-1, 0, -1),
    (1, 0, -1), (-1, 0, 1), (0, 1, 1), (0, -1, -1), (0, 1, -1), (0, -1, 1),
]
TO_REF = [REFERENCE_VEL.index(v) for v in VEL]
OPP = [VEL.index((-x, -y, -z)) for x, y, z in VEL]
WEIGHT = [(1.0 / 3.0, 1.0 / 18.0, 1.0 / 36.0)[abs(x) + abs(y) + abs(z)] for x, y, z in VEL]
DIRECTIONS = [(1, 0), (-1, 0), (0, 1), (0, -1), (1, 1), (1, -1), (-1, 1), (-1, -1)]


def pieces(dx, dy, sizes):
    lx, ly = sizes

    def beyond(d, length, near, far):
        return (-far if d > 0 else length - 1 + near, far - near + 1)

    def x(near, far=None):
        return beyond(dx, lx, near, far or near)

    def y(near, far=None):
        return beyond(dy, ly, near, far or near)

    def one(cx, cy):
        return VEL.index((cx, cy, 0)), 1

    every = (0, 19)
    if dy == 0:
        cells = [
            (1, every, x(1), (0, ly)),
            (1, every, x(2, 3), (0, 1)),
            (1, every, x(2, 3), (ly - 1, 1)),
            (1, one(dx, -1), x(4), (0, 1)),
            (1, one(dx, 1), x(4), (ly - 1, 1)),
            (2, every, x(2), (1, ly - 2)),
            (2, one(dx, -1), x(3), (1, 1)),
            (2, one(dx, 1), x(3), (ly - 2, 1)),
        ]
    elif dx == 0:
        cells = [
            (1, every, (0, lx), y(1)),
            (1, every, (0, 1), y(2, 3)),
            (1, every, (lx - 1, 1), y(2, 3)),
            (1, one(-1, dy), (0, 1), y(4)),
            (1, one(1, dy), (lx - 1, 1), y(4)),
            (2, every, (1, lx - 2), y(2)),
            (2, one(-1, dy), (1, 1), y(3)),
            (2, one(1, dy), (lx - 2, 1), y(3)),
        ]
    else:
        cells = [
            (1, every, x(1), y(1, 3)),
            (1, every, x(2, 3), y(1)),
            (1, one(dx, dy), x(4), y(1)),
            (1, one(dx, dy), x(1), y(4)),
            (2, every, x(2), y(2)),
            (2, one(dx, dy), x(3), y(2)),
            (2, one(dx, dy), x(2), y(3)),
        ]
    return [(level, lo, n, layers, rows) for level, (lo, n), layers, rows in cells]


def place(a, b, sizes):
    lx, ly = sizes
    bx = (a >= lx) - (a < 0)
    by = (b >= ly) - (b < 0)
    a, b = a - bx * lx, b - by * ly
    return (bx, by), min(a + 1, lx - a, b + 1, ly - b, 2)


def linked(time, sizes):
    def rule(x, y):
        if time > 2:
            return True
        block, level = place(*x, sizes)
        other, beneath = place(*y, sizes)
        return block != other or block == (0, 0) or level < time or beneath < time

    return rule


def linked_inside(time, sizes):
    def rule(x, y):
        block, level = place(*y, sizes)
        return block == (0, 0) and level >= time

    return rule


def collide(f):
    pairs = [(q, OPP[q]) for q in range(1, 19) if q < OPP[q]]
    rho = f[0]
    moment = [None, None, None]
    for i, j in pairs:
        rho = rho + (f[i] + f[j])
        diff = f[i] - f[j]
        for axis in range(3):
            c = VEL[i][axis]
            if c:
                term = moment[axis]
                if term is None:
                    moment[axis] = diff if c > 0 else -diff
                else:
                    moment[axis] = term + diff if c > 0 else term - diff
    inverse = 1.0 / rho
    u = [m * inverse for m in moment]
    base = 1.0 - 1.5 * (u[0] * u[0] + u[1] * u[1] + u[2] * u[2])
    scaled = {w: (RELAX * w) * rho for w in set(WEIGHT)}
    keep = 1.0 - RELAX
    post = [None] * 19
    post[0] = keep * f[0] + scaled[WEIGHT[0]] * base
    for i, j in pairs:
        proj = None
        for axis in range(3):
            c = VEL[i][axis]
            if c:
                if proj is None:
                    proj = u[axis] if c > 0 else -u[axis]
                else:
                    proj = proj + u[axis] if c > 0 else proj - u[axis]
        even = scaled[WEIGHT[i]] * (base + 4.5 * (proj * proj))
        odd = scaled[WEIGHT[i]] * (3.0 * proj)
        post[i] = keep * f[i] + (even + odd)
        post[j] = keep * f[j] + (even - odd)
    return post


def stream(buf, corner, a, row, rule):
    layer, base = corner[0] + a, corner[1] + row
    shape = (8, buf.shape[-1])
    rows = lax.broadcasted_iota(jnp.int32, shape, 0)
    masks = {}

    def open_rows(pattern):
        if pattern not in masks:
            mask = None
            start = 0
            while start < 8:
                if pattern[start]:
                    end = start
                    while end < 8 and pattern[end]:
                        end += 1
                    part = None
                    if start > 0:
                        part = rows >= start
                    if end < 8:
                        part = rows < end if part is None else part & (rows < end)
                    mask = part if mask is None else mask | part
                    start = end
                else:
                    start += 1
            masks[pattern] = mask
        return masks[pattern]

    result = []
    for q, (cx, cy, cz) in enumerate(VEL):
        kept = buf[OPP[q], layer, base : base + 8, :]
        pattern = tuple(rule((a, row + r), (a - cx, row + r - cy)) for r in range(8))
        if q == 0 or not any(pattern):
            result.append(kept)
            continue
        source = buf[q, layer - cx, base - cy : base - cy + 8, :]
        if cz:
            source = pltpu.roll(source, cz % source.shape[-1], 1)
        carry = source == source
        if not all(pattern):
            carry = carry & open_rows(pattern)
        result.append(jnp.where(carry, source, kept))
    return result


def kernel(axes, sizes, pops_hbm, fluid_hbm, out, first, wet, own1, own2, s1, s2, p1, p2, p3, p4, *sems):
    in_sem, send_sem, recv_sem, late_sem = sems
    lx, ly = sizes
    nx, ny = axes
    ix, iy = lax.axis_index("gx"), lax.axis_index("gy")
    has = {0: None, 1: iy < ny - 1, -1: iy > 0}
    lanes = first.shape[-1]
    solid = jnp.full((ly, lanes), jnp.nan, jnp.float32)

    def when(condition, action):
        if condition is None:
            action()
        else:
            pl.when(condition)(action)

    def target(dx, dy):
        return {"gx": lax.rem(ix + nx + dx, nx), "gy": iy + dy}

    fluid_in = pltpu.make_async_copy(fluid_hbm, wet, in_sem.at[lx])
    loads = [
        pltpu.make_async_copy(pops_hbm.at[:, a], first.at[:, a], in_sem.at[a]) for a in range(lx)
    ]

    barrier = pltpu.get_barrier_semaphore()
    is_first, is_last = ix == 0, ix == nx - 1
    columns = 1 + (iy > 0).astype(jnp.int32) + (iy < ny - 1).astype(jnp.int32)

    def greet(sem, dx, dy):
        pl.semaphore_signal(
            sem, inc=1, device_id=target(dx, dy), device_id_type=pl.DeviceIdType.MESH
        )

    for dx, dy in DIRECTIONS:
        condition = has[dy]
        if dx > 0:
            condition = ix < nx - 2 if condition is None else jnp.logical_and(condition, ix < nx - 2)
        when(condition, lambda dx=dx, dy=dy: greet(barrier, dx, dy))

    def wait_barrier():
        ends = jnp.logical_or(is_first, is_last)
        pl.semaphore_wait(barrier, jnp.where(ends, 2, 3) * columns - 1)

        @pl.when(ix >= nx - 2)
        def _():
            for dy in (0, 1, -1):
                when(has[dy], lambda dy=dy: greet(late_sem, 1, dy))

    def fill_walls():
        for edge, row in ((iy == 0, PAD - 8), (iy == ny - 1, PAD + ly)):

            @pl.when(edge)
            def _():
                for q in range(19):
                    for a in range(lx + 2 * HALO):
                        p1[q, a, row : row + 8, :] = jnp.full((8, lanes), jnp.nan, jnp.float32)

    def message(level, dx, dy, nearest=None):
        source, into = ((s1, p1), (s2, p2))[level - 1]
        base = sum(len(pieces(*d, sizes)) for d in DIRECTIONS[: DIRECTIONS.index((dx, dy))])
        copies = []
        for i, (at, lo, n, (a, an), (b, bn)) in enumerate(pieces(dx, dy, sizes)):
            seam = an == 1 and a in (-1, lx)
            if at == level and nearest in (None, seam):
                copies.append(
                    pltpu.make_async_remote_copy(
                        src_ref=source.at[pl.ds(lo, n), pl.ds(a + dx * lx, an), pl.ds(b + dy * ly, bn)],
                        dst_ref=into.at[pl.ds(lo, n), pl.ds(HALO + a, an), pl.ds(PAD + b, bn)],
                        send_sem=send_sem.at[base + i],
                        recv_sem=recv_sem.at[base + i],
                        device_id=target(dx, dy),
                        device_id_type=pl.DeviceIdType.MESH,
                    )
                )
        return copies

    def each(dy, copies, action):
        when(has[dy], lambda: [getattr(c, action)() for c in copies] and None)

    def post_layer(a):
        loads[a].wait()
        f = [first[TO_REF[q], a] for q in range(19)]
        f[0] = jnp.where(wet[a] != 0, f[0], solid)
        for q, value in enumerate(collide(f)):
            own1[q, a, PAD : PAD + ly, :] = value
            p1[q, HALO + a, PAD : PAD + ly, :] = value

    def part(source, into, a, time):
        f = stream(source, (0, PAD), a, 0, linked_inside(time, sizes))
        for q, value in enumerate(f):
            into[OPP[q], a] = jnp.where(wet[a] != 0, value, solid)
        return f

    def part_layer(a):
        f = part(own1, s1, a, 1)
        if 0 < a < lx - 1:
            for q, value in enumerate(collide(f)):
                own2[q, a, PAD : PAD + ly, :] = value

    def advance(source, into, time, a, row, lo=0, hi=8):
        f = stream(source, (HALO, PAD), a, row, linked(time, sizes))
        for q, value in enumerate(collide(f)):
            into[q, HALO + a, PAD + row + lo : PAD + row + hi, :] = value[lo:hi]

    def rows(ring):
        return sorted({-ring, ly + ring - 8})

    def second(a):
        if a in (-1, 0, lx - 1, lx):
            for row in rows(3):
                advance(p1, p2, 1, a, row)
        elif 0 < a < lx - 1:
            for row in rows(1):
                advance(p1, p2, 1, a, row)
        else:
            advance(p1, p2, 1, a, -1, 0, 2)
            advance(p1, p2, 1, a, ly - 7, 6, 8)

    def variant(side):
        ys = (0, 1, -1)
        away, home = [(side, dy) for dy in ys], [(-side, dy) for dy in ys]
        across = [(0, 1), (0, -1)]
        order = [a if side < 0 else lx - 1 - a for a in range(lx)]

        def layers(lo, hi):
            return [a if side < 0 else lx - 1 - a for a in range(lo, hi + 1)]

        fluid_in.start()
        for a in order:
            loads[a].start()
        fill_walls()
        fluid_in.wait()
        post_layer(order[0])
        post_layer(order[1])
        part_layer(order[0])
        wait_barrier()

        def send(directions, level, nearest=None):
            for d in directions:
                each(d[1], message(level, *d, nearest), "start")

        if side < 0:
            pl.when(jnp.logical_not(is_first))(lambda: send(away, 1, True))
        else:
            send(away, 1, True)
        for a in order[2:]:
            post_layer(a)
        for a in order[1:]:
            part_layer(a)
        if side < 0:
            pl.when(jnp.logical_not(is_first))(lambda: send(away, 1, False))
            send(across, 1)
            send(home, 1)
        else:
            send(away, 1, False)
            send(across, 1)
            pl.when(jnp.logical_not(is_last))(lambda: send(home, 1))
        for a in order[1:-1]:
            part(own2, s2, a, 2)
        if side < 0:
            pl.when(jnp.logical_not(is_first))(lambda: send(away, 2))
            send(across, 2)
            send(home, 2)

            @pl.when(is_first)
            def _():
                pl.semaphore_wait(late_sem, columns)
                send(away, 1)
                send(away, 2)
        else:
            send(away, 2)
            send(across, 2)
            pl.when(jnp.logical_not(is_last))(lambda: send(home, 2))

            @pl.when(is_last)
            def _():
                pl.semaphore_wait(late_sem, columns)
                send(home, 1)
                send(home, 2)

        def receive(directions, level):
            for d in directions:
                each(-d[1], message(level, *d), "wait_recv")

        receive(across, 1)
        receive(away, 1)
        for a in layers(1, lx + 2):
            second(a)
        receive(across, 2)
        receive(away, 2)
        for a in layers(2, lx + 1):
            for row in rows(2):
                advance(p2, p3, 2, a, row)
        for a in layers(3, lx):
            for row in rows(1):
                advance(p3, p4, 3, a, row)
        receive(home, 1)
        for a in layers(-3, 0):
            second(a)
        receive(home, 2)
        for a in layers(-2, 1):
            for row in rows(2):
                advance(p2, p3, 2, a, row)
        for a in layers(-1, 2):
            for row in rows(1):
                advance(p3, p4, 3, a, row)

    pl.when(lax.rem(ix, 2) == 0)(lambda: variant(-1))
    pl.when(lax.rem(ix, 2) == 1)(lambda: variant(1))
    for a in range(lx):
        f = stream(p4, (HALO, PAD), a, 0, linked(4, sizes))
        for q in range(19):
            out[TO_REF[q], a] = jnp.where(wet[a] != 0, f[q], first[TO_REF[q], a])
    for level in (1, 2):
        for d in DIRECTIONS:
            each(d[1], message(level, *d), "wait_send")


def write_out(source, target, sem):
    copies = [
        pltpu.make_async_copy(source.at[:, a], target.at[:, a], sem.at[a])
        for a in range(source.shape[1])
    ]
    for copy in copies:
        copy.start()
    for copy in copies:
        copy.wait()


def per_device(axes, populations, fluid):
    sizes = fluid.shape[:2]
    lx, ly = sizes
    nz = fluid.shape[2]
    count = sum(len(pieces(dx, dy, sizes)) for dx, dy in DIRECTIONS)
    dma = pltpu.SemaphoreType.DMA
    block = pltpu.VMEM(populations.shape, jnp.float32)
    tall = pltpu.VMEM((19, lx, ly + 2 * PAD, nz), jnp.float32)
    wide = pltpu.VMEM((19, lx + 2 * HALO, ly + 2 * PAD, nz), jnp.float32)
    result = pl.pallas_call(
        functools.partial(kernel, axes, sizes),
        out_shape=pltpu.VMEM(populations.shape, populations.dtype),
        in_specs=[pl.BlockSpec(memory_space=pl.ANY)] * 2,
        out_specs=pl.BlockSpec(memory_space=pltpu.VMEM),
        scratch_shapes=[block, pltpu.VMEM(fluid.shape, jnp.int32), tall, tall, block, block]
        + [wide] * STEPS
        + [dma((lx + 1,)), dma((count,)), dma((count,)), pltpu.SemaphoreType.REGULAR],
        compiler_params=pltpu.CompilerParams(
            collective_id=0, has_side_effects=True, vmem_limit_bytes=60 * 1024 * 1024
        ),
    )(populations, fluid)
    return pl.pallas_call(
        write_out,
        out_shape=jax.ShapeDtypeStruct(populations.shape, populations.dtype),
        in_specs=[pl.BlockSpec(memory_space=pltpu.VMEM)],
        out_specs=pl.BlockSpec(memory_space=pl.ANY),
        scratch_shapes=[dma((lx,))],
        compiler_params=pltpu.CompilerParams(vmem_limit_bytes=16 * 2**20),
    )(result)


def solution(mesh):
    axes = (mesh.shape["gx"], mesh.shape["gy"])
    return jax.shard_map(
        functools.partial(per_device, axes),
        mesh=mesh,
        in_specs=(P(None, "gx", "gy", None), P("gx", "gy", None)),
        out_specs=P(None, "gx", "gy", None),
        check_vma=False,
    )
```

```python
import functools

import jax
import jax.numpy as jnp
import numpy as np
from jax import lax
from jax.experimental import pallas as pl
from jax.experimental.pallas import tpu as pltpu
from jax.sharding import PartitionSpec as P

STEPS = 4
HALO = 4
PAD = 8
RELAX = 1.25

VEL = [
    (0, 0, 0), (0, 0, 1), (0, 0, -1),
    (0, -1, 0), (0, -1, 1), (0, -1, -1),
    (0, 1, 0), (0, 1, 1), (0, 1, -1),
    (1, 1, 0), (1, 0, 0), (1, 0, 1), (1, 0, -1), (1, -1, 0),
    (-1, -1, 0), (-1, 0, 0), (-1, 0, 1), (-1, 0, -1), (-1, 1, 0),
]
REFERENCE_VEL = [
    (0, 0, 0), (1, 0, 0), (-1, 0, 0), (0, 1, 0), (0, -1, 0), (0, 0, 1), (0, 0, -1),
    (1, 1, 0), (-1, -1, 0), (1, -1, 0), (-1, 1, 0), (1, 0, 1), (-1, 0, -1),
    (1, 0, -1), (-1, 0, 1), (0, 1, 1), (0, -1, -1), (0, 1, -1), (0, -1, 1),
]
TO_REF = [REFERENCE_VEL.index(v) for v in VEL]
OPP = [VEL.index((-x, -y, -z)) for x, y, z in VEL]
WEIGHT = [(1.0 / 3.0, 1.0 / 18.0, 1.0 / 36.0)[abs(x) + abs(y) + abs(z)] for x, y, z in VEL]
DIRECTIONS = [(1, 0), (-1, 0), (0, 1), (0, -1), (1, 1), (1, -1), (-1, 1), (-1, -1)]


def pieces(dx, dy, sizes):
    lx, ly = sizes

    def beyond(d, length, near, far):
        return (-far if d > 0 else length - 1 + near, far - near + 1)

    def x(near, far=None):
        return beyond(dx, lx, near, far or near)

    def y(near, far=None):
        return beyond(dy, ly, near, far or near)

    def one(cx, cy):
        return VEL.index((cx, cy, 0)), 1

    every = (0, 19)
    if dy == 0:
        cells = [
            (1, every, x(1), (0, ly)),
            (1, every, x(2, 3), (0, 1)),
            (1, every, x(2, 3), (ly - 1, 1)),
            (1, one(dx, -1), x(4), (0, 1)),
            (1, one(dx, 1), x(4), (ly - 1, 1)),
            (2, every, x(2), (1, ly - 2)),
            (2, one(dx, -1), x(3), (1, 1)),
            (2, one(dx, 1), x(3), (ly - 2, 1)),
        ]
    elif dx == 0:
        cells = [
            (1, every, (0, lx), y(1)),
            (1, every, (0, 1), y(2, 3)),
            (1, every, (lx - 1, 1), y(2, 3)),
            (1, one(-1, dy), (0, 1), y(4)),
            (1, one(1, dy), (lx - 1, 1), y(4)),
            (2, every, (1, lx - 2), y(2)),
            (2, one(-1, dy), (1, 1), y(3)),
            (2, one(1, dy), (lx - 2, 1), y(3)),
        ]
    else:
        cells = [
            (1, every, x(1), y(1, 3)),
            (1, every, x(2, 3), y(1)),
            (1, one(dx, dy), x(4), y(1)),
            (1, one(dx, dy), x(1), y(4)),
            (2, every, x(2), y(2)),
            (2, one(dx, dy), x(3), y(2)),
            (2, one(dx, dy), x(2), y(3)),
        ]
    return [(level, lo, n, layers, rows) for level, (lo, n), layers, rows in cells]


def place(a, b, sizes):
    lx, ly = sizes
    bx = (a >= lx) - (a < 0)
    by = (b >= ly) - (b < 0)
    a, b = a - bx * lx, b - by * ly
    return (bx, by), min(a + 1, lx - a, b + 1, ly - b, 2)


def linked(time, sizes):
    def rule(x, y):
        if time > 2:
            return True
        block, level = place(*x, sizes)
        other, beneath = place(*y, sizes)
        return block != other or block == (0, 0) or level < time or beneath < time

    return rule


def linked_inside(time, sizes):
    def rule(x, y):
        block, level = place(*y, sizes)
        return block == (0, 0) and level >= time

    return rule


def collide(f):
    pairs = [(q, OPP[q]) for q in range(1, 19) if q < OPP[q]]
    rho = f[0]
    moment = [None, None, None]
    for i, j in pairs:
        rho = rho + (f[i] + f[j])
        diff = f[i] - f[j]
        for axis in range(3):
            c = VEL[i][axis]
            if c:
                term = moment[axis]
                if term is None:
                    moment[axis] = diff if c > 0 else -diff
                else:
                    moment[axis] = term + diff if c > 0 else term - diff
    inverse = 1.0 / rho
    u = [m * inverse for m in moment]
    base = 1.0 - 1.5 * (u[0] * u[0] + u[1] * u[1] + u[2] * u[2])
    scaled = {w: (RELAX * w) * rho for w in set(WEIGHT)}
    keep = 1.0 - RELAX
    post = [None] * 19
    post[0] = keep * f[0] + scaled[WEIGHT[0]] * base
    for i, j in pairs:
        proj = None
        for axis in range(3):
            c = VEL[i][axis]
            if c:
                if proj is None:
                    proj = u[axis] if c > 0 else -u[axis]
                else:
                    proj = proj + u[axis] if c > 0 else proj - u[axis]
        even = scaled[WEIGHT[i]] * (base + 4.5 * (proj * proj))
        odd = scaled[WEIGHT[i]] * (3.0 * proj)
        post[i] = keep * f[i] + (even + odd)
        post[j] = keep * f[j] + (even - odd)
    return post


def stream(buf, corner, a, row, rule):
    layer, base = corner[0] + a, corner[1] + row
    shape = (8, buf.shape[-1])
    rows = lax.broadcasted_iota(jnp.int32, shape, 0)
    masks = {}

    def open_rows(pattern):
        if pattern not in masks:
            mask = None
            start = 0
            while start < 8:
                if pattern[start]:
                    end = start
                    while end < 8 and pattern[end]:
                        end += 1
                    part = None
                    if start > 0:
                        part = rows >= start
                    if end < 8:
                        part = rows < end if part is None else part & (rows < end)
                    mask = part if mask is None else mask | part
                    start = end
                else:
                    start += 1
            masks[pattern] = mask
        return masks[pattern]

    result = []
    for q, (cx, cy, cz) in enumerate(VEL):
        kept = buf[OPP[q], layer, base : base + 8, :]
        pattern = tuple(rule((a, row + r), (a - cx, row + r - cy)) for r in range(8))
        if q == 0 or not any(pattern):
            result.append(kept)
            continue
        source = buf[q, layer - cx, base - cy : base - cy + 8, :]
        if cz:
            source = pltpu.roll(source, cz % source.shape[-1], 1)
        carry = source == source
        if not all(pattern):
            carry = carry & open_rows(pattern)
        result.append(jnp.where(carry, source, kept))
    return result


def kernel(axes, sizes, pops_hbm, fluid_hbm, out, first, wet, own1, own2, s1, s2, p1, p2, p3, p4, *sems):
    tally, in_sem, send_sem, recv_sem, late_sem = sems
    lx, ly = sizes
    nx, ny = axes
    ix, iy = lax.axis_index("gx"), lax.axis_index("gy")
    has = {0: None, 1: iy < ny - 1, -1: iy > 0}
    lanes = first.shape[-1]
    solid = jnp.full((ly, lanes), jnp.nan, jnp.float32)

    def when(condition, action):
        if condition is None:
            action()
        else:
            pl.when(condition)(action)

    def target(dx, dy):
        return {"gx": lax.rem(ix + nx + dx, nx), "gy": iy + dy}

    fluid_in = pltpu.make_async_copy(fluid_hbm, wet, in_sem.at[lx])
    loads = [
        pltpu.make_async_copy(pops_hbm.at[:, a], first.at[:, a], in_sem.at[a]) for a in range(lx)
    ]

    barrier = pltpu.get_barrier_semaphore()
    is_first, is_last = ix == 0, ix == nx - 1
    columns = 1 + (iy > 0).astype(jnp.int32) + (iy < ny - 1).astype(jnp.int32)

    def greet(sem, dx, dy):
        pl.semaphore_signal(
            sem, inc=1, device_id=target(dx, dy), device_id_type=pl.DeviceIdType.MESH
        )

    for dx, dy in DIRECTIONS:
        condition = has[dy]
        if dx > 0:
            condition = ix < nx - 2 if condition is None else jnp.logical_and(condition, ix < nx - 2)
        when(condition, lambda dx=dx, dy=dy: greet(barrier, dx, dy))

    def wait_barrier():
        ends = jnp.logical_or(is_first, is_last)
        pl.semaphore_wait(barrier, jnp.where(ends, 2, 3) * columns - 1)

        @pl.when(ix >= nx - 2)
        def _():
            for dy in (0, 1, -1):
                when(has[dy], lambda dy=dy: greet(late_sem, 1, dy))

    def fill_walls():
        for edge, row in ((iy == 0, PAD - 8), (iy == ny - 1, PAD + ly)):

            @pl.when(edge)
            def _():
                for q in range(19):
                    for a in range(lx + 2 * HALO):
                        p1[q, a, row : row + 8, :] = jnp.full((8, lanes), jnp.nan, jnp.float32)

    def message(side, level, dx, dy, nearest=None):
        source, into = ((s1, p1), (s2, p2))[level - 1]
        copies = []
        for at, lo, n, (a, an), (b, bn) in pieces(dx, dy, sizes):
            seam = an == 1 and a in (-1, lx)
            if at == level and nearest in (None, seam):
                copies.append(
                    pltpu.make_async_remote_copy(
                        src_ref=source.at[pl.ds(lo, n), pl.ds(a + dx * lx, an), pl.ds(b + dy * ly, bn)],
                        dst_ref=into.at[pl.ds(lo, n), pl.ds(HALO + a, an), pl.ds(PAD + b, bn)],
                        send_sem=send_sem.at[dy + 1],
                        recv_sem=recv_sem.at[int(dx == side), level - 1, dy + 1],
                        device_id=target(dx, dy),
                        device_id_type=pl.DeviceIdType.MESH,
                    )
                )
        return copies

    def amount(directions, levels):
        return sum(
            n * an * bn
            for d in directions
            for at, lo, n, (a, an), (b, bn) in pieces(*d, sizes)
            if at in levels
        )

    def await_rows(sem, count):
        pltpu.make_async_copy(tally.at[pl.ds(0, count)], tally.at[pl.ds(0, count)], sem).wait()

    def post_layer(a):
        loads[a].wait()
        f = [first[TO_REF[q], a] for q in range(19)]
        f[0] = jnp.where(wet[a] != 0, f[0], solid)
        for q, value in enumerate(collide(f)):
            own1[q, a, PAD : PAD + ly, :] = value
            p1[q, HALO + a, PAD : PAD + ly, :] = value

    def part(source, into, a, time):
        f = stream(source, (0, PAD), a, 0, linked_inside(time, sizes))
        for q, value in enumerate(f):
            into[OPP[q], a] = jnp.where(wet[a] != 0, value, solid)
        return f

    def part_layer(a):
        f = part(own1, s1, a, 1)
        if 0 < a < lx - 1:
            for q, value in enumerate(collide(f)):
                own2[q, a, PAD : PAD + ly, :] = value

    def advance(source, into, time, a, row, lo=0, hi=8):
        f = stream(source, (HALO, PAD), a, row, linked(time, sizes))
        for q, value in enumerate(collide(f)):
            into[q, HALO + a, PAD + row + lo : PAD + row + hi, :] = value[lo:hi]

    def rows(ring):
        return sorted({-ring, ly + ring - 8})

    def second(a):
        if a in (-1, 0, lx - 1, lx):
            for row in rows(3):
                advance(p1, p2, 1, a, row)
        elif 0 < a < lx - 1:
            for row in rows(1):
                advance(p1, p2, 1, a, row)
        else:
            advance(p1, p2, 1, a, -1, 0, 2)
            advance(p1, p2, 1, a, ly - 7, 6, 8)

    def variant(side):
        ys = (0, 1, -1)
        away, home = [(side, dy) for dy in ys], [(-side, dy) for dy in ys]
        across = [(0, 1), (0, -1)]
        order = [a if side < 0 else lx - 1 - a for a in range(lx)]

        def layers(lo, hi):
            return [a if side < 0 else lx - 1 - a for a in range(lo, hi + 1)]

        fluid_in.start()
        for a in order:
            loads[a].start()
        fill_walls()
        fluid_in.wait()
        post_layer(order[0])
        post_layer(order[1])
        part_layer(order[0])
        wait_barrier()

        def send(directions, level, nearest=None):
            for d in directions:
                copies = message(side, level, *d, nearest)
                when(has[d[1]], lambda copies=copies: [c.start() for c in copies] and None)

        if side < 0:
            pl.when(jnp.logical_not(is_first))(lambda: send(away, 1, True))
        else:
            send(away, 1, True)
        for a in order[2:]:
            post_layer(a)
        for a in order[1:]:
            part_layer(a)
        if side < 0:
            pl.when(jnp.logical_not(is_first))(lambda: send(away, 1, False))
            send(across, 1)
            send(home, 1)
        else:
            send(away, 1, False)
            send(across, 1)
            pl.when(jnp.logical_not(is_last))(lambda: send(home, 1))
        for a in order[1:-1]:
            part(own2, s2, a, 2)
        if side < 0:
            pl.when(jnp.logical_not(is_first))(lambda: send(away, 2))
            send(across, 2)
            send(home, 2)

            @pl.when(is_first)
            def _():
                pl.semaphore_wait(late_sem, columns)
                send(away, 1)
                send(away, 2)
        else:
            send(away, 2)
            send(across, 2)
            pl.when(jnp.logical_not(is_last))(lambda: send(home, 2))

            @pl.when(is_last)
            def _():
                pl.semaphore_wait(late_sem, columns)
                send(home, 1)
                send(home, 2)

        def receive(late, level):
            dx = -side if late else side
            for dy in (0, 1, -1):
                directions = [(dx, dy)] if late or dy == 0 else [(dx, dy), (0, dy)]
                when(
                    has[-dy],
                    lambda dy=dy, count=amount(directions, (level,)): await_rows(
                        recv_sem.at[int(late), level - 1, dy + 1], count
                    ),
                )

        receive(False, 1)
        for a in layers(1, lx + 2):
            second(a)
        receive(False, 2)
        for a in layers(2, lx + 1):
            for row in rows(2):
                advance(p2, p3, 2, a, row)
        for a in layers(3, lx):
            for row in rows(1):
                advance(p3, p4, 3, a, row)
        receive(True, 1)
        for a in layers(-3, 0):
            second(a)
        receive(True, 2)
        for a in layers(-2, 1):
            for row in rows(2):
                advance(p2, p3, 2, a, row)
        for a in layers(-1, 2):
            for row in rows(1):
                advance(p3, p4, 3, a, row)

    pl.when(lax.rem(ix, 2) == 0)(lambda: variant(-1))
    pl.when(lax.rem(ix, 2) == 1)(lambda: variant(1))
    for a in range(lx):
        f = stream(p4, (HALO, PAD), a, 0, linked(4, sizes))
        for q in range(19):
            out[TO_REF[q], a] = jnp.where(wet[a] != 0, f[q], first[TO_REF[q], a])
    for dy in (0, 1, -1):
        count = amount([d for d in DIRECTIONS if d[1] == dy], (1, 2))
        when(has[dy], lambda dy=dy, count=count: await_rows(send_sem.at[dy + 1], count))


def write_out(source, target, sem):
    copies = [
        pltpu.make_async_copy(source.at[:, a], target.at[:, a], sem.at[a])
        for a in range(source.shape[1])
    ]
    for copy in copies:
        copy.start()
    for copy in copies:
        copy.wait()


def per_device(axes, populations, fluid):
    sizes = fluid.shape[:2]
    lx, ly = sizes
    nz = fluid.shape[2]
    count = sum(n * a[1] * b[1] for d in DIRECTIONS for _, _, n, a, b in pieces(*d, sizes))
    dma = pltpu.SemaphoreType.DMA
    block = pltpu.VMEM(populations.shape, jnp.float32)
    tall = pltpu.VMEM((19, lx, ly + 2 * PAD, nz), jnp.float32)
    wide = pltpu.VMEM((19, lx + 2 * HALO, ly + 2 * PAD, nz), jnp.float32)
    result = pl.pallas_call(
        functools.partial(kernel, axes, sizes),
        out_shape=pltpu.VMEM(populations.shape, populations.dtype),
        in_specs=[pl.BlockSpec(memory_space=pl.ANY)] * 2,
        out_specs=pl.BlockSpec(memory_space=pltpu.VMEM),
        scratch_shapes=[block, pltpu.VMEM(fluid.shape, jnp.int32), tall, tall, block, block]
        + [wide] * STEPS
        + [pltpu.VMEM((count, nz), jnp.float32)]
        + [dma((lx + 1,)), dma((3,)), dma((2, 2, 3)), pltpu.SemaphoreType.REGULAR],
        compiler_params=pltpu.CompilerParams(
            collective_id=0, has_side_effects=True, vmem_limit_bytes=60 * 1024 * 1024
        ),
    )(populations, fluid)
    return pl.pallas_call(
        write_out,
        out_shape=jax.ShapeDtypeStruct(populations.shape, populations.dtype),
        in_specs=[pl.BlockSpec(memory_space=pltpu.VMEM)],
        out_specs=pl.BlockSpec(memory_space=pl.ANY),
        scratch_shapes=[dma((lx,))],
        compiler_params=pltpu.CompilerParams(vmem_limit_bytes=16 * 2**20),
    )(result)


def solution(mesh):
    axes = (mesh.shape["gx"], mesh.shape["gy"])
    return jax.shard_map(
        functools.partial(per_device, axes),
        mesh=mesh,
        in_specs=(P(None, "gx", "gy", None), P("gx", "gy", None)),
        out_specs=P(None, "gx", "gy", None),
        check_vma=False,
    )
```

```python
import functools

import jax
import jax.numpy as jnp
import numpy as np
from jax import lax
from jax.experimental import pallas as pl
from jax.experimental.pallas import tpu as pltpu
from jax.sharding import PartitionSpec as P

STEPS = 4
HALO = 4
PAD = 8
RELAX = 1.25

VEL = [
    (0, 0, 0), (0, 0, 1), (0, 0, -1),
    (0, -1, 0), (0, -1, 1), (0, -1, -1),
    (0, 1, 0), (0, 1, 1), (0, 1, -1),
    (1, 1, 0), (1, 0, 0), (1, 0, 1), (1, 0, -1), (1, -1, 0),
    (-1, -1, 0), (-1, 0, 0), (-1, 0, 1), (-1, 0, -1), (-1, 1, 0),
]
REFERENCE_VEL = [
    (0, 0, 0), (1, 0, 0), (-1, 0, 0), (0, 1, 0), (0, -1, 0), (0, 0, 1), (0, 0, -1),
    (1, 1, 0), (-1, -1, 0), (1, -1, 0), (-1, 1, 0), (1, 0, 1), (-1, 0, -1),
    (1, 0, -1), (-1, 0, 1), (0, 1, 1), (0, -1, -1), (0, 1, -1), (0, -1, 1),
]
TO_REF = [REFERENCE_VEL.index(v) for v in VEL]
OPP = [VEL.index((-x, -y, -z)) for x, y, z in VEL]
WEIGHT = [(1.0 / 3.0, 1.0 / 18.0, 1.0 / 36.0)[abs(x) + abs(y) + abs(z)] for x, y, z in VEL]
DIRECTIONS = [(1, 0), (-1, 0), (0, 1), (0, -1), (1, 1), (1, -1), (-1, 1), (-1, -1)]


def pieces(dx, dy, sizes):
    lx, ly = sizes

    def beyond(d, length, near, far):
        return (-far if d > 0 else length - 1 + near, far - near + 1)

    def x(near, far=None):
        return beyond(dx, lx, near, far or near)

    def y(near, far=None):
        return beyond(dy, ly, near, far or near)

    def one(cx, cy):
        return VEL.index((cx, cy, 0)), 1

    every = (0, 19)
    if dy == 0:
        cells = [
            (1, every, x(1), (0, ly)),
            (1, every, x(2, 3), (0, 1)),
            (1, every, x(2, 3), (ly - 1, 1)),
            (1, one(dx, -1), x(4), (0, 1)),
            (1, one(dx, 1), x(4), (ly - 1, 1)),
            (2, every, x(2), (1, ly - 2)),
            (2, one(dx, -1), x(3), (1, 1)),
            (2, one(dx, 1), x(3), (ly - 2, 1)),
        ]
    elif dx == 0:
        cells = [
            (1, every, (0, lx), y(1)),
            (1, every, (0, 1), y(2, 3)),
            (1, every, (lx - 1, 1), y(2, 3)),
            (1, one(-1, dy), (0, 1), y(4)),
            (1, one(1, dy), (lx - 1, 1), y(4)),
            (2, every, (1, lx - 2), y(2)),
            (2, one(-1, dy), (1, 1), y(3)),
            (2, one(1, dy), (lx - 2, 1), y(3)),
        ]
    else:
        cells = [
            (1, every, x(1), y(1, 3)),
            (1, every, x(2, 3), y(1)),
            (1, one(dx, dy), x(4), y(1)),
            (1, one(dx, dy), x(1), y(4)),
            (2, every, x(2), y(2)),
            (2, one(dx, dy), x(3), y(2)),
            (2, one(dx, dy), x(2), y(3)),
        ]
    return [(level, lo, n, layers, rows) for level, (lo, n), layers, rows in cells]


def place(a, b, sizes):
    lx, ly = sizes
    bx = (a >= lx) - (a < 0)
    by = (b >= ly) - (b < 0)
    a, b = a - bx * lx, b - by * ly
    return (bx, by), min(a + 1, lx - a, b + 1, ly - b, 2)


def linked(time, sizes):
    def rule(x, y):
        if time > 2:
            return True
        block, level = place(*x, sizes)
        other, beneath = place(*y, sizes)
        return block != other or block == (0, 0) or level < time or beneath < time

    return rule


def linked_inside(time, sizes):
    def rule(x, y):
        block, level = place(*y, sizes)
        return block == (0, 0) and level >= time

    return rule


def collide(f):
    pairs = [(q, OPP[q]) for q in range(1, 19) if q < OPP[q]]
    rho = f[0]
    moment = [None, None, None]
    for i, j in pairs:
        rho = rho + (f[i] + f[j])
        diff = f[i] - f[j]
        for axis in range(3):
            c = VEL[i][axis]
            if c:
                term = moment[axis]
                if term is None:
                    moment[axis] = diff if c > 0 else -diff
                else:
                    moment[axis] = term + diff if c > 0 else term - diff
    inverse = 1.0 / rho
    u = [m * inverse for m in moment]
    base = 1.0 - 1.5 * (u[0] * u[0] + u[1] * u[1] + u[2] * u[2])
    scaled = {w: (RELAX * w) * rho for w in set(WEIGHT)}
    keep = 1.0 - RELAX
    post = [None] * 19
    post[0] = keep * f[0] + scaled[WEIGHT[0]] * base
    for i, j in pairs:
        proj = None
        for axis in range(3):
            c = VEL[i][axis]
            if c:
                if proj is None:
                    proj = u[axis] if c > 0 else -u[axis]
                else:
                    proj = proj + u[axis] if c > 0 else proj - u[axis]
        even = scaled[WEIGHT[i]] * (base + 4.5 * (proj * proj))
        odd = scaled[WEIGHT[i]] * (3.0 * proj)
        post[i] = keep * f[i] + (even + odd)
        post[j] = keep * f[j] + (even - odd)
    return post


def stream(buf, corner, a, row, rule):
    layer, base = corner[0] + a, corner[1] + row
    shape = (8, buf.shape[-1])
    rows = lax.broadcasted_iota(jnp.int32, shape, 0)
    masks = {}

    def open_rows(pattern):
        if pattern not in masks:
            mask = None
            start = 0
            while start < 8:
                if pattern[start]:
                    end = start
                    while end < 8 and pattern[end]:
                        end += 1
                    part = None
                    if start > 0:
                        part = rows >= start
                    if end < 8:
                        part = rows < end if part is None else part & (rows < end)
                    mask = part if mask is None else mask | part
                    start = end
                else:
                    start += 1
            masks[pattern] = mask
        return masks[pattern]

    result = []
    for q, (cx, cy, cz) in enumerate(VEL):
        kept = buf[OPP[q], layer, base : base + 8, :]
        pattern = tuple(rule((a, row + r), (a - cx, row + r - cy)) for r in range(8))
        if q == 0 or not any(pattern):
            result.append(kept)
            continue
        source = buf[q, layer - cx, base - cy : base - cy + 8, :]
        if cz:
            source = pltpu.roll(source, cz % source.shape[-1], 1)
        carry = source == source
        if not all(pattern):
            carry = carry & open_rows(pattern)
        result.append(jnp.where(carry, source, kept))
    return result


def kernel(axes, sizes, pops_hbm, fluid_hbm, out, first, wet, own1, own2, s1, s2, p1, p2, p3, p4, *sems):
    tally, in_sem, send_sem, recv_sem, late_sem = sems
    lx, ly = sizes
    nx, ny = axes
    ix, iy = lax.axis_index("gx"), lax.axis_index("gy")
    has = {0: None, 1: iy < ny - 1, -1: iy > 0}
    lanes = first.shape[-1]
    solid = jnp.full((ly, lanes), jnp.nan, jnp.float32)

    def when(condition, action):
        if condition is None:
            action()
        else:
            pl.when(condition)(action)

    def target(dx, dy):
        return {"gx": lax.rem(ix + nx + dx, nx), "gy": iy + dy}

    fluid_in = pltpu.make_async_copy(fluid_hbm, wet, in_sem.at[lx])
    loads = [
        pltpu.make_async_copy(pops_hbm.at[:, a], first.at[:, a], in_sem.at[a]) for a in range(lx)
    ]

    barrier = pltpu.get_barrier_semaphore()
    is_first, is_last = ix == 0, ix == nx - 1
    columns = 1 + (iy > 0).astype(jnp.int32) + (iy < ny - 1).astype(jnp.int32)

    def greet(sem, dx, dy):
        pl.semaphore_signal(
            sem, inc=1, device_id=target(dx, dy), device_id_type=pl.DeviceIdType.MESH
        )

    for dx, dy in DIRECTIONS:
        condition = has[dy]
        if dx > 0:
            condition = ix < nx - 2 if condition is None else jnp.logical_and(condition, ix < nx - 2)
        when(condition, lambda dx=dx, dy=dy: greet(barrier, dx, dy))

    def wait_barrier():
        ends = jnp.logical_or(is_first, is_last)
        pl.semaphore_wait(barrier, jnp.where(ends, 2, 3) * columns - 1)

        @pl.when(ix >= nx - 2)
        def _():
            for dy in (0, 1, -1):
                when(has[dy], lambda dy=dy: greet(late_sem, 1, dy))

    def fill_walls():
        for edge, row in ((iy == 0, PAD - 8), (iy == ny - 1, PAD + ly)):

            @pl.when(edge)
            def _():
                for q in range(19):
                    for a in range(lx + 2 * HALO):
                        p1[q, a, row : row + 8, :] = jnp.full((8, lanes), jnp.nan, jnp.float32)

    def message(side, level, dx, dy, nearest=None):
        source, into = ((s1, p1), (s2, p2))[level - 1]
        copies = []
        for at, lo, n, (a, an), (b, bn) in pieces(dx, dy, sizes):
            seam = an == 1 and a in (-1, lx)
            if at == level and nearest in (None, seam):
                copies.append(
                    pltpu.make_async_remote_copy(
                        src_ref=source.at[pl.ds(lo, n), pl.ds(a + dx * lx, an), pl.ds(b + dy * ly, bn)],
                        dst_ref=into.at[pl.ds(lo, n), pl.ds(HALO + a, an), pl.ds(PAD + b, bn)],
                        send_sem=send_sem,
                        recv_sem=recv_sem.at[(int(dx == side) if dx else 2), level - 1],
                        device_id=target(dx, dy),
                        device_id_type=pl.DeviceIdType.MESH,
                    )
                )
        return copies

    def forward(side, level, dy):
        buf = (p1, p2)[level - 1]
        return [
            pltpu.make_async_remote_copy(
                src_ref=buf.at[pl.ds(lo, n), pl.ds(HALO + a - side * lx, an), pl.ds(PAD + b, bn)],
                dst_ref=buf.at[pl.ds(lo, n), pl.ds(HALO + a, an), pl.ds(PAD + b, bn)],
                send_sem=send_sem,
                recv_sem=recv_sem.at[0, level - 1],
                device_id=target(-side, 0),
                device_id_type=pl.DeviceIdType.MESH,
            )
            for at, lo, n, (a, an), (b, bn) in pieces(-side, dy, sizes)
            if at == level
        ]

    def amount(directions, levels):
        return sum(
            n * an * bn
            for d in directions
            for at, lo, n, (a, an), (b, bn) in pieces(*d, sizes)
            if at in levels
        )

    def await_rows(sem, count):
        pltpu.make_async_copy(tally.at[pl.ds(0, count)], tally.at[pl.ds(0, count)], sem).wait()

    def await_by_sides(sem, base, extra):
        for sides in range(3):
            if base + sides * extra:
                count = base + sides * extra
                pl.when(columns == 1 + sides)(lambda count=count: await_rows(sem, count))

    def post_layer(a):
        loads[a].wait()
        f = [first[TO_REF[q], a] for q in range(19)]
        f[0] = jnp.where(wet[a] != 0, f[0], solid)
        for q, value in enumerate(collide(f)):
            own1[q, a, PAD : PAD + ly, :] = value
            p1[q, HALO + a, PAD : PAD + ly, :] = value

    def part(source, into, a, time):
        f = stream(source, (0, PAD), a, 0, linked_inside(time, sizes))
        for q, value in enumerate(f):
            into[OPP[q], a] = jnp.where(wet[a] != 0, value, solid)
        return f

    def part_layer(a):
        f = part(own1, s1, a, 1)
        if 0 < a < lx - 1:
            for q, value in enumerate(collide(f)):
                own2[q, a, PAD : PAD + ly, :] = value

    def advance(source, into, time, a, row, lo=0, hi=8):
        f = stream(source, (HALO, PAD), a, row, linked(time, sizes))
        for q, value in enumerate(collide(f)):
            into[q, HALO + a, PAD + row + lo : PAD + row + hi, :] = value[lo:hi]

    def rows(ring):
        return sorted({-ring, ly + ring - 8})

    def second(a):
        if a in (-1, 0, lx - 1, lx):
            for row in rows(3):
                advance(p1, p2, 1, a, row)
        elif 0 < a < lx - 1:
            for row in rows(1):
                advance(p1, p2, 1, a, row)
        else:
            advance(p1, p2, 1, a, -1, 0, 2)
            advance(p1, p2, 1, a, ly - 7, 6, 8)

    def third(layers):
        for a in layers:
            for row in rows(2):
                advance(p2, p3, 2, a, row)

    def fourth(layers):
        for a in layers:
            for row in rows(1):
                advance(p3, p4, 3, a, row)

    def last(layers):
        for a in layers:
            f = stream(p4, (HALO, PAD), a, 0, linked(4, sizes))
            for q in range(19):
                out[TO_REF[q], a] = jnp.where(wet[a] != 0, f[q], first[TO_REF[q], a])

    def variant(side):
        ys = (-1, 0, 1)
        away, home = [(side, dy) for dy in ys], [(-side, 0)]
        across = [(0, 1), (0, -1)]
        order = [a if side < 0 else lx - 1 - a for a in range(lx)]

        def layers(lo, hi):
            return [a if side < 0 else lx - 1 - a for a in range(lo, hi + 1)]

        fluid_in.start()
        for a in order:
            loads[a].start()
        fill_walls()
        fluid_in.wait()
        post_layer(order[0])
        post_layer(order[1])
        part_layer(order[0])
        wait_barrier()

        def send(directions, level, nearest=None):
            for d in directions:
                copies = message(side, level, *d, nearest)
                when(has[d[1]], lambda copies=copies: [c.start() for c in copies] and None)

        if side < 0:
            pl.when(jnp.logical_not(is_first))(lambda: send(away, 1, True))
        else:
            send(away, 1, True)
        for a in order[2:]:
            post_layer(a)
        for a in order[1:]:
            part_layer(a)
        if side < 0:
            pl.when(jnp.logical_not(is_first))(lambda: send(away, 1, False))
        else:
            send(away, 1, False)
        for a in order[1:-1]:
            part(own2, s2, a, 2)
        if side < 0:
            pl.when(jnp.logical_not(is_first))(lambda: send(away, 2))
            for level in (1, 2):
                send(across + home, level)

        else:
            send(away, 2)
            for level in (1, 2):
                send(across, level)
                pl.when(jnp.logical_not(is_last))(lambda level=level: send(home, level))

            @pl.when(is_last)
            def _():
                pl.semaphore_wait(late_sem, columns)
                send(home, 1)
                send(home, 2)

        def receive(late, level):
            dx = -side if late else side
            await_by_sides(
                recv_sem.at[int(late), level - 1],
                amount([(dx, 0)], (level,)),
                amount([(dx, 1)], (level,)),
            )

        if side < 0:

            @pl.when(is_first)
            def _():
                pl.semaphore_wait(late_sem, columns)
                send(away, 1)
                send(away, 2)

        for level in (1, 2):
            await_by_sides(recv_sem.at[2, level - 1], 0, amount([(0, 1)], (level,)))
            for dy in (1, -1):
                copies = forward(side, level, dy)
                when(has[-dy], lambda copies=copies: [c.start() for c in copies] and None)
        receive(False, 1)
        for a in layers(1, lx + 2):
            second(a)
        receive(False, 2)
        third(layers(2, lx + 1))
        fourth(layers(3, lx))
        receive(True, 1)
        for a in layers(-3, 0):
            second(a)
        third(layers(0, 1))
        fourth(layers(1, 2))
        last(layers(2, lx - 1))
        receive(True, 2)
        third(layers(-2, -1))
        fourth(layers(-1, 0))
        last(layers(0, 1))

    pl.when(lax.rem(ix, 2) == 0)(lambda: variant(-1))
    pl.when(lax.rem(ix, 2) == 1)(lambda: variant(1))
    await_by_sides(
        send_sem,
        amount([d for d in DIRECTIONS if d[1] == 0], (1, 2)),
        amount([d for d in DIRECTIONS if d[1] == 1], (1, 2)),
    )


def write_out(source, target, sem):
    copy = pltpu.make_async_copy(source, target, sem)
    copy.start()
    copy.wait()


def per_device(axes, populations, fluid):
    sizes = fluid.shape[:2]
    lx, ly = sizes
    nz = fluid.shape[2]
    count = sum(n * a[1] * b[1] for d in DIRECTIONS for _, _, n, a, b in pieces(*d, sizes))
    dma = pltpu.SemaphoreType.DMA
    block = pltpu.VMEM(populations.shape, jnp.float32)
    tall = pltpu.VMEM((19, lx, ly + 2 * PAD, nz), jnp.float32)
    wide = pltpu.VMEM((19, lx + 2 * HALO, ly + 2 * PAD, nz), jnp.float32)
    result = pl.pallas_call(
        functools.partial(kernel, axes, sizes),
        out_shape=pltpu.VMEM(populations.shape, populations.dtype),
        in_specs=[pl.BlockSpec(memory_space=pl.ANY)] * 2,
        out_specs=pl.BlockSpec(memory_space=pltpu.VMEM),
        scratch_shapes=[block, pltpu.VMEM(fluid.shape, jnp.int32), tall, tall, block, block]
        + [wide] * STEPS
        + [pltpu.VMEM((count, nz), jnp.float32)]
        + [dma((lx + 1,)), dma, dma((3, 2)), pltpu.SemaphoreType.REGULAR],
        compiler_params=pltpu.CompilerParams(
            collective_id=0, has_side_effects=True, vmem_limit_bytes=60 * 1024 * 1024
        ),
    )(populations, fluid)
    return pl.pallas_call(
        write_out,
        out_shape=jax.ShapeDtypeStruct(populations.shape, populations.dtype),
        in_specs=[pl.BlockSpec(memory_space=pltpu.VMEM)],
        out_specs=pl.BlockSpec(memory_space=pl.ANY),
        scratch_shapes=[dma],
        compiler_params=pltpu.CompilerParams(vmem_limit_bytes=16 * 2**20),
    )(result)


def solution(mesh):
    axes = (mesh.shape["gx"], mesh.shape["gy"])
    return jax.shard_map(
        functools.partial(per_device, axes),
        mesh=mesh,
        in_specs=(P(None, "gx", "gy", None), P("gx", "gy", None)),
        out_specs=P(None, "gx", "gy", None),
        check_vma=False,
    )
```

```python
import functools

import jax
import jax.numpy as jnp
import numpy as np
from jax import lax
from jax.experimental import pallas as pl
from jax.experimental.pallas import tpu as pltpu
from jax.sharding import PartitionSpec as P

STEPS = 4
HALO = 4
PAD = 8
RELAX = 1.25

VEL = [
    (0, 0, 0), (0, 0, 1), (0, 0, -1),
    (0, -1, 0), (0, -1, 1), (0, -1, -1),
    (0, 1, 0), (0, 1, 1), (0, 1, -1),
    (1, 1, 0), (1, 0, 0), (1, 0, 1), (1, 0, -1), (1, -1, 0),
    (-1, -1, 0), (-1, 0, 0), (-1, 0, 1), (-1, 0, -1), (-1, 1, 0),
]
REFERENCE_VEL = [
    (0, 0, 0), (1, 0, 0), (-1, 0, 0), (0, 1, 0), (0, -1, 0), (0, 0, 1), (0, 0, -1),
    (1, 1, 0), (-1, -1, 0), (1, -1, 0), (-1, 1, 0), (1, 0, 1), (-1, 0, -1),
    (1, 0, -1), (-1, 0, 1), (0, 1, 1), (0, -1, -1), (0, 1, -1), (0, -1, 1),
]
TO_REF = [REFERENCE_VEL.index(v) for v in VEL]
OPP = [VEL.index((-x, -y, -z)) for x, y, z in VEL]
WEIGHT = [(1.0 / 3.0, 1.0 / 18.0, 1.0 / 36.0)[abs(x) + abs(y) + abs(z)] for x, y, z in VEL]
DIRECTIONS = [(1, 0), (-1, 0), (0, 1), (0, -1), (1, 1), (1, -1), (-1, 1), (-1, -1)]


def pieces(dx, dy, sizes):
    lx, ly = sizes

    def beyond(d, length, near, far):
        return (-far if d > 0 else length - 1 + near, far - near + 1)

    def x(near, far=None):
        return beyond(dx, lx, near, far or near)

    def y(near, far=None):
        return beyond(dy, ly, near, far or near)

    def one(cx, cy):
        return VEL.index((cx, cy, 0)), 1

    every = (0, 19)
    if dy == 0:
        cells = [
            (1, every, x(1), (0, ly)),
            (1, every, x(2, 3), (0, 1)),
            (1, every, x(2, 3), (ly - 1, 1)),
            (1, one(dx, -1), x(4), (0, 1)),
            (1, one(dx, 1), x(4), (ly - 1, 1)),
            (2, every, x(2), (1, ly - 2)),
            (2, one(dx, -1), x(3), (1, 1)),
            (2, one(dx, 1), x(3), (ly - 2, 1)),
        ]
    elif dx == 0:
        cells = [
            (1, every, (0, lx), y(1)),
            (1, every, (0, 1), y(2, 3)),
            (1, every, (lx - 1, 1), y(2, 3)),
            (1, one(-1, dy), (0, 1), y(4)),
            (1, one(1, dy), (lx - 1, 1), y(4)),
            (2, every, (1, lx - 2), y(2)),
            (2, one(-1, dy), (1, 1), y(3)),
            (2, one(1, dy), (lx - 2, 1), y(3)),
        ]
    else:
        cells = [
            (1, every, x(1), y(1, 3)),
            (1, every, x(2, 3), y(1)),
            (1, one(dx, dy), x(4), y(1)),
            (1, one(dx, dy), x(1), y(4)),
            (2, every, x(2), y(2)),
            (2, one(dx, dy), x(3), y(2)),
            (2, one(dx, dy), x(2), y(3)),
        ]
    return [(level, lo, n, layers, rows) for level, (lo, n), layers, rows in cells]


def place(a, b, sizes):
    lx, ly = sizes
    bx = (a >= lx) - (a < 0)
    by = (b >= ly) - (b < 0)
    a, b = a - bx * lx, b - by * ly
    return (bx, by), min(a + 1, lx - a, b + 1, ly - b, 2)


def linked(time, sizes):
    def rule(x, y):
        if time > 2:
            return True
        block, level = place(*x, sizes)
        other, beneath = place(*y, sizes)
        return block != other or block == (0, 0) or level < time or beneath < time

    return rule


def linked_inside(time, sizes):
    def rule(x, y):
        block, level = place(*y, sizes)
        return block == (0, 0) and level >= time

    return rule


def collide(f):
    pairs = [(q, OPP[q]) for q in range(1, 19) if q < OPP[q]]
    rho = f[0]
    moment = [None, None, None]
    for i, j in pairs:
        rho = rho + (f[i] + f[j])
        diff = f[i] - f[j]
        for axis in range(3):
            c = VEL[i][axis]
            if c:
                term = moment[axis]
                if term is None:
                    moment[axis] = diff if c > 0 else -diff
                else:
                    moment[axis] = term + diff if c > 0 else term - diff
    inverse = 1.0 / rho
    u = [m * inverse for m in moment]
    base = 1.0 - 1.5 * (u[0] * u[0] + u[1] * u[1] + u[2] * u[2])
    level = {w: ((RELAX * w) * rho) * base for w in sorted(set(WEIGHT))}
    slope = {w: (3.0 * RELAX * w) * rho for w in sorted(set(WEIGHT[1:]))}
    keep = 1.0 - RELAX
    post = [None] * 19
    post[0] = keep * f[0] + level[WEIGHT[0]]
    for i, j in pairs:
        proj = None
        for axis in range(3):
            c = VEL[i][axis]
            if c:
                if proj is None:
                    proj = u[axis] if c > 0 else -u[axis]
                else:
                    proj = proj + u[axis] if c > 0 else proj - u[axis]
        odd = slope[WEIGHT[i]] * proj
        even = level[WEIGHT[i]] + (1.5 * proj) * odd
        post[i] = keep * f[i] + (even + odd)
        post[j] = keep * f[j] + (even - odd)
    return post


def stream(buf, corner, a, row, rule):
    layer, base = corner[0] + a, corner[1] + row
    shape = (8, buf.shape[-1])
    rows = lax.broadcasted_iota(jnp.int32, shape, 0)
    masks = {}

    def open_rows(pattern):
        if pattern not in masks:
            mask = None
            start = 0
            while start < 8:
                if pattern[start]:
                    end = start
                    while end < 8 and pattern[end]:
                        end += 1
                    part = None
                    if start > 0:
                        part = rows >= start
                    if end < 8:
                        part = rows < end if part is None else part & (rows < end)
                    mask = part if mask is None else mask | part
                    start = end
                else:
                    start += 1
            masks[pattern] = mask
        return masks[pattern]

    result = []
    for q, (cx, cy, cz) in enumerate(VEL):
        kept = buf[OPP[q], layer, base : base + 8, :]
        pattern = tuple(rule((a, row + r), (a - cx, row + r - cy)) for r in range(8))
        if q == 0 or not any(pattern):
            result.append(kept)
            continue
        source = buf[q, layer - cx, base - cy : base - cy + 8, :]
        if cz:
            source = pltpu.roll(source, cz % source.shape[-1], 1)
        carry = source == source
        if not all(pattern):
            carry = carry & open_rows(pattern)
        result.append(jnp.where(carry, source, kept))
    return result


def kernel(axes, sizes, pops_hbm, fluid_hbm, out, first, wet, own1, own2, s1, s2, p1, p2, p3, p4, *sems):
    tally, in_sem, send_sem, recv_sem, late_sem = sems
    lx, ly = sizes
    nx, ny = axes
    ix, iy = lax.axis_index("gx"), lax.axis_index("gy")
    has = {0: None, 1: iy < ny - 1, -1: iy > 0}
    lanes = first.shape[-1]
    solid = jnp.full((ly, lanes), jnp.nan, jnp.float32)

    def when(condition, action):
        if condition is None:
            action()
        else:
            pl.when(condition)(action)

    def target(dx, dy):
        return {"gx": lax.rem(ix + nx + dx, nx), "gy": iy + dy}

    fluid_in = pltpu.make_async_copy(fluid_hbm, wet, in_sem.at[lx])
    loads = [
        pltpu.make_async_copy(pops_hbm.at[:, a], first.at[:, a], in_sem.at[a]) for a in range(lx)
    ]

    barrier = pltpu.get_barrier_semaphore()
    is_first, is_last = ix == 0, ix == nx - 1
    columns = 1 + (iy > 0).astype(jnp.int32) + (iy < ny - 1).astype(jnp.int32)

    def greet(sem, dx, dy):
        pl.semaphore_signal(
            sem, inc=1, device_id=target(dx, dy), device_id_type=pl.DeviceIdType.MESH
        )

    for dx, dy in DIRECTIONS:
        condition = has[dy]
        if dx > 0:
            condition = ix < nx - 2 if condition is None else jnp.logical_and(condition, ix < nx - 2)
        when(condition, lambda dx=dx, dy=dy: greet(barrier, dx, dy))

    def wait_barrier():
        ends = jnp.logical_or(is_first, is_last)
        pl.semaphore_wait(barrier, jnp.where(ends, 2, 3) * columns - 1)

        @pl.when(ix >= nx - 2)
        def _():
            for dy in (0, 1, -1):
                when(has[dy], lambda dy=dy: greet(late_sem, 1, dy))

    def fill_walls():
        for edge, row in ((iy == 0, PAD - 8), (iy == ny - 1, PAD + ly)):

            @pl.when(edge)
            def _():
                for q in range(19):
                    for a in range(lx + 2 * HALO):
                        p1[q, a, row : row + 8, :] = jnp.full((8, lanes), jnp.nan, jnp.float32)

    def message(side, level, dx, dy, nearest=None):
        source, into = ((s1, p1), (s2, p2))[level - 1]
        copies = []
        for at, lo, n, (a, an), (b, bn) in pieces(dx, dy, sizes):
            seam = an == 1 and a in (-1, lx)
            if at == level and nearest in (None, seam):
                copies.append(
                    pltpu.make_async_remote_copy(
                        src_ref=source.at[pl.ds(lo, n), pl.ds(a + dx * lx, an), pl.ds(b + dy * ly, bn)],
                        dst_ref=into.at[pl.ds(lo, n), pl.ds(HALO + a, an), pl.ds(PAD + b, bn)],
                        send_sem=send_sem,
                        recv_sem=recv_sem.at[(int(dx == side) if dx else 2), level - 1],
                        device_id=target(dx, dy),
                        device_id_type=pl.DeviceIdType.MESH,
                    )
                )
        return copies

    def forward(side, level, dy):
        buf = (p1, p2)[level - 1]
        return [
            pltpu.make_async_remote_copy(
                src_ref=buf.at[pl.ds(lo, n), pl.ds(HALO + a - side * lx, an), pl.ds(PAD + b, bn)],
                dst_ref=buf.at[pl.ds(lo, n), pl.ds(HALO + a, an), pl.ds(PAD + b, bn)],
                send_sem=send_sem,
                recv_sem=recv_sem.at[0, level - 1],
                device_id=target(-side, 0),
                device_id_type=pl.DeviceIdType.MESH,
            )
            for at, lo, n, (a, an), (b, bn) in pieces(-side, dy, sizes)
            if at == level
        ]

    def amount(directions, levels):
        return sum(
            n * an * bn
            for d in directions
            for at, lo, n, (a, an), (b, bn) in pieces(*d, sizes)
            if at in levels
        )

    def await_rows(sem, count):
        pltpu.make_async_copy(tally.at[pl.ds(0, count)], tally.at[pl.ds(0, count)], sem).wait()

    def await_by_sides(sem, base, extra):
        for sides in range(3):
            if base + sides * extra:
                count = base + sides * extra
                pl.when(columns == 1 + sides)(lambda count=count: await_rows(sem, count))

    def post_layer(a):
        loads[a].wait()
        f = [first[TO_REF[q], a] for q in range(19)]
        f[0] = jnp.where(wet[a] != 0, f[0], solid)
        for q, value in enumerate(collide(f)):
            own1[q, a, PAD : PAD + ly, :] = value
            p1[q, HALO + a, PAD : PAD + ly, :] = value

    def part(source, into, a, time):
        f = stream(source, (0, PAD), a, 0, linked_inside(time, sizes))
        for q, value in enumerate(f):
            into[OPP[q], a] = jnp.where(wet[a] != 0, value, solid)
        return f

    def part_layer(a):
        f = part(own1, s1, a, 1)
        if 0 < a < lx - 1:
            for q, value in enumerate(collide(f)):
                own2[q, a, PAD : PAD + ly, :] = value

    def advance(source, into, time, a, row, lo=0, hi=8):
        f = stream(source, (HALO, PAD), a, row, linked(time, sizes))
        for q, value in enumerate(collide(f)):
            into[q, HALO + a, PAD + row + lo : PAD + row + hi, :] = value[lo:hi]

    def rows(ring):
        return sorted({-ring, ly + ring - 8})

    def second(a):
        if a in (-1, 0, lx - 1, lx):
            for row in rows(3):
                advance(p1, p2, 1, a, row)
        elif 0 < a < lx - 1:
            for row in rows(1):
                advance(p1, p2, 1, a, row)
        else:
            advance(p1, p2, 1, a, -1, 0, 2)
            advance(p1, p2, 1, a, ly - 7, 6, 8)

    def third(layers):
        for a in layers:
            for row in rows(2):
                advance(p2, p3, 2, a, row)

    def fourth(layers):
        for a in layers:
            for row in rows(1):
                advance(p3, p4, 3, a, row)

    def last(layers):
        for a in layers:
            f = stream(p4, (HALO, PAD), a, 0, linked(4, sizes))
            for q in range(19):
                out[TO_REF[q], a] = jnp.where(wet[a] != 0, f[q], first[TO_REF[q], a])

    def variant(side):
        ys = (-1, 0, 1)
        away, home = [(side, dy) for dy in ys], [(-side, 0)]
        across = [(0, 1), (0, -1)]
        order = [a if side < 0 else lx - 1 - a for a in range(lx)]

        def layers(lo, hi):
            return [a if side < 0 else lx - 1 - a for a in range(lo, hi + 1)]

        fluid_in.start()
        for a in order:
            loads[a].start()
        fill_walls()
        fluid_in.wait()
        post_layer(order[0])
        post_layer(order[1])
        part_layer(order[0])
        wait_barrier()

        def send(directions, level, nearest=None):
            for d in directions:
                copies = message(side, level, *d, nearest)
                when(has[d[1]], lambda copies=copies: [c.start() for c in copies] and None)

        free = jnp.logical_not(is_first) if side < 0 else ix >= 0
        down, face, up = [(side, -1)], [(side, 0)], [(side, 1)]

        def leading(level, nearest=None):
            pl.when(free)(lambda: send(down, level, nearest))

        def facing(level, nearest=None):
            pl.when(jnp.logical_and(free, iy == 0))(lambda: send(face, level, nearest))

        leading(1, True)
        facing(1, True)
        for a in order[2:]:
            post_layer(a)
        for a in order[1:]:
            part_layer(a)
        leading(1, False)
        facing(1, False)
        for a in order[1:-1]:
            part(own2, s2, a, 2)
        leading(2)
        pl.when(jnp.logical_and(free, iy > 0))(lambda: send(face, 1))
        pl.when(free)(lambda: (send(face, 2), send(up, 1), send(up, 2), None)[3])
        if side < 0:
            for level in (1, 2):
                send(across + home, level)

        else:
            for level in (1, 2):
                send(across, level)
                pl.when(jnp.logical_not(is_last))(lambda level=level: send(home, level))

            @pl.when(is_last)
            def _():
                pl.semaphore_wait(late_sem, columns)
                send(home, 1)
                send(home, 2)

        def receive(late, level):
            dx = -side if late else side
            await_by_sides(
                recv_sem.at[int(late), level - 1],
                amount([(dx, 0)], (level,)),
                amount([(dx, 1)], (level,)),
            )

        if side < 0:

            @pl.when(is_first)
            def _():
                pl.semaphore_wait(late_sem, columns)
                send(away, 1)
                send(away, 2)

        for level in (1, 2):
            await_by_sides(recv_sem.at[2, level - 1], 0, amount([(0, 1)], (level,)))
            for dy in (1, -1):
                copies = forward(side, level, dy)
                when(has[-dy], lambda copies=copies: [c.start() for c in copies] and None)
        receive(False, 1)
        for a in layers(1, lx + 2):
            second(a)
        receive(False, 2)
        third(layers(2, lx + 1))
        fourth(layers(3, lx))
        receive(True, 1)
        for a in layers(-3, 0):
            second(a)
        third(layers(0, 1))
        fourth(layers(1, 2))
        last(layers(2, lx - 1))
        receive(True, 2)
        third(layers(-2, -1))
        fourth(layers(-1, 0))
        last(layers(0, 1))

    pl.when(lax.rem(ix, 2) == 0)(lambda: variant(-1))
    pl.when(lax.rem(ix, 2) == 1)(lambda: variant(1))
    await_by_sides(
        send_sem,
        amount([d for d in DIRECTIONS if d[1] == 0], (1, 2)),
        amount([d for d in DIRECTIONS if d[1] == 1], (1, 2)),
    )


def write_out(source, target, sem):
    copy = pltpu.make_async_copy(source, target, sem)
    copy.start()
    copy.wait()


def per_device(axes, populations, fluid):
    sizes = fluid.shape[:2]
    lx, ly = sizes
    nz = fluid.shape[2]
    count = sum(n * a[1] * b[1] for d in DIRECTIONS for _, _, n, a, b in pieces(*d, sizes))
    dma = pltpu.SemaphoreType.DMA
    block = pltpu.VMEM(populations.shape, jnp.float32)
    tall = pltpu.VMEM((19, lx, ly + 2 * PAD, nz), jnp.float32)
    wide = pltpu.VMEM((19, lx + 2 * HALO, ly + 2 * PAD, nz), jnp.float32)
    result = pl.pallas_call(
        functools.partial(kernel, axes, sizes),
        out_shape=pltpu.VMEM(populations.shape, populations.dtype),
        in_specs=[pl.BlockSpec(memory_space=pl.ANY)] * 2,
        out_specs=pl.BlockSpec(memory_space=pltpu.VMEM),
        scratch_shapes=[block, pltpu.VMEM(fluid.shape, jnp.int32), tall, tall, block, block]
        + [wide] * STEPS
        + [pltpu.VMEM((count, nz), jnp.float32)]
        + [dma((lx + 1,)), dma, dma((3, 2)), pltpu.SemaphoreType.REGULAR],
        compiler_params=pltpu.CompilerParams(
            collective_id=0, has_side_effects=True, vmem_limit_bytes=60 * 1024 * 1024
        ),
    )(populations, fluid)
    return pl.pallas_call(
        write_out,
        out_shape=jax.ShapeDtypeStruct(populations.shape, populations.dtype),
        in_specs=[pl.BlockSpec(memory_space=pltpu.VMEM)],
        out_specs=pl.BlockSpec(memory_space=pl.ANY),
        scratch_shapes=[dma],
        compiler_params=pltpu.CompilerParams(vmem_limit_bytes=16 * 2**20),
    )(result)


def solution(mesh):
    axes = (mesh.shape["gx"], mesh.shape["gy"])
    return jax.shard_map(
        functools.partial(per_device, axes),
        mesh=mesh,
        in_specs=(P(None, "gx", "gy", None), P("gx", "gy", None)),
        out_specs=P(None, "gx", "gy", None),
        check_vma=False,
    )
```
